128 devices in a mesh: lon: 32 (over x, y, z_hi), lev: 4 (over z_lo, core).
Axes of the slice: x: 4, y: 4, z: 4 (z_hi: 2, z_lo: 2; z = z_hi * 2 + z_lo), core: 2. Of those that a mesh axis runs over, the one named last changes fastest.
Arguments:
- field: float32 [72, 512, 128], P('lev', 'lon'), may hold values from -6 to 6
- ens: bfloat16 [80, 72, 512, 128], P(None, 'lev', 'lon'), may hold values from -2 to 2
- sdev: float32 [72, 512, 128], P('lev', 'lon'), may hold values from 0.5 to 2
- lon_taper: bfloat16 [17], replicated, may hold values from 0 to 0.079589844
- static_taper: bfloat16 [17], replicated, may hold values from 0 to 0.079589844
- loc_vert: bfloat16 [72, 72], P('lev'), may hold values from -0.75 to 0.75
- static_vert: bfloat16 [72, 72], P('lev'), may hold values from -0.75 to 0.75
- obs_block: int32 [32768], P('lon'), may hold values from -1 to 511, as said below
- obs_value: float32 [32768], P('lon'), may hold values from -6 to 6
- obs_rinv: float32 [32768], P('lon'), may hold values from 0.25 to 4
- obs_horiz: float32 [32768, 128], P('lon'), may hold values from -0.5 to 0.5
- obs_vert: float32 [32768, 72], P('lon', 'lev'), may hold values from -0.75 to 0.75
Outputs:
- increment: float32 [72, 512, 128], P('lev', 'lon')
- adjoint_field: float32 [72, 512, 128], P('lev', 'lon')
- obs_cost: float32 [], replicated
The draws below stay inside these ranges and needn't reach their ends.
Inputs may be any that keep to these rules, and one draw needn't show every extreme that they name: `obs_block`: each longitude sector's 1024 slots name only blocks within that sector's longitudes; live slots come first, in non-falling block order; at least half of a sector's slots are live, and some sector has all its slots live.
All inputs are finite; a program needn't handle non-finite values.
Results may differ from the reference program's by a relative error of at most 0.0041.
Values may be sent and summed in bfloat16 or wider, within the bound.
A program may use at most 128 MiB of HBM per device.

```python
import math
import jax
import jax.numpy as jnp
from jax import lax

ENS = 80
LEV = 72
LAT = 128
LON_DEV = 16
OBS_DEV = 1024
HALO = 8
NLON = 512
NOBS = 32768


def draw_obs_block(key, part):
    groups = NOBS // OBS_DEV
    per_group = LON_DEV // 8 * (LAT // 16)
    key_ids = jax.random.fold_in(key, 11)
    key_live = jax.random.fold_in(key, 23)
    local = jnp.sort(jax.random.randint(key_ids, (groups, OBS_DEV), 0, per_group), axis=1)
    counts = jax.random.randint(key_live, (groups, 1), OBS_DEV // 2, OBS_DEV + 1)
    counts = counts.at[0, 0].set(OBS_DEV)
    slots = jnp.arange(OBS_DEV)[None, :]
    base = jnp.arange(groups)[:, None] * per_group
    ids = jnp.where(slots < counts, local + base, -1)
    return ids.reshape(-1).astype(jnp.int32)


def steps_of(stream_key, dims, shards, least, high):
    level, own = 1.0, jax.random.fold_in(stream_key, 6)
    for position, blocks in shards:
        steps = jnp.exp(jax.random.uniform(jax.random.fold_in(own, position), (blocks,), jnp.float32, least / len(shards), high / len(shards)))
        level = level * jnp.repeat(steps, dims[position] // blocks).reshape([-1 if axis == position else 1 for axis in range(len(dims))])
    return level


def noise(rng, dims, spread, most, cuts=(), dtype=jnp.bfloat16):
    entries = spread * jax.random.normal(rng, dims, jnp.float32)
    if cuts:
        entries = entries * steps_of(rng, dims, cuts, -0.22, 0.18)
    return jnp.clip(entries, -most, most).astype(dtype)


def setup_inputs(seed: int = 0) -> dict:
    key_list = jax.random.split(jax.random.key(seed), 13)
    field = noise(key_list[0], (LEV, NLON, LAT), 1.0, 6.0, ((0, 4), (1, 32)), jnp.float32)
    ens = noise(key_list[1], (ENS, LEV, NLON, LAT), 0.3, 2.0, ((1, 4), (2, 32)))
    sdev = jnp.clip(jnp.exp(math.log(2.0) - 1.3862944 * jax.random.uniform(key_list[2], (LEV, NLON, LAT), jnp.float32) ** steps_of(key_list[2], (LEV, NLON, LAT), ((0, 4), (1, 32)), -0.2, 0.2)), 0.5, 2.0)
    lon_taper = jnp.clip(jax.random.uniform(key_list[3], (2 * HALO + 1,), jnp.float32, 0.0, 0.079589844), 0.0, 0.079589844).astype(jnp.bfloat16)
    static_taper = jnp.clip(jax.random.uniform(key_list[4], (2 * HALO + 1,), jnp.float32, 0.0, 0.079589844), 0.0, 0.079589844).astype(jnp.bfloat16)
    loc_vert = noise(key_list[5], (LEV, LEV), LEV ** -0.5, 0.75, ((0, 4),))
    static_vert = noise(key_list[6], (LEV, LEV), LEV ** -0.5, 0.75, ((0, 4),))
    obs_block = draw_obs_block(jax.random.fold_in(key_list[12], 71), 0)
    obs_value = noise(key_list[8], (NOBS,), 1.0, 6.0, ((0, 32),), jnp.float32)
    obs_rinv = jnp.clip(jnp.exp(math.log(4.0) - 2.7725887 * jax.random.uniform(key_list[9], (NOBS,), jnp.float32) ** steps_of(key_list[9], (NOBS,), ((0, 32),), -0.2, 0.2)), 0.25, 4.0)
    obs_horiz = noise(key_list[10], (NOBS, 128), 128 ** -0.5, 0.5, ((0, 32),), jnp.float32)
    obs_vert = noise(key_list[11], (NOBS, LEV), LEV ** -0.5, 0.75, ((0, 32), (1, 4)), jnp.float32)
    return dict(field=field, ens=ens, sdev=sdev, lon_taper=lon_taper, static_taper=static_taper, loc_vert=loc_vert, static_vert=static_vert, obs_block=obs_block, obs_value=obs_value, obs_rinv=obs_rinv, obs_horiz=obs_horiz, obs_vert=obs_vert)


ens_weight = 0.8
static_weight = 0.5


def localize(zfield, taper, vmatrix):
    width = taper.shape[0]
    half = width // 2
    total = jnp.zeros(zfield.shape, jnp.float32)
    for offset in range(width):
        total = total + taper[offset].astype(jnp.float32) * jnp.roll(zfield, half - offset, axis=1).astype(jnp.float32)
    smooth = total.astype(jnp.bfloat16)
    levels = smooth.shape[0]
    flat = smooth.reshape(levels, -1)
    return jnp.dot(vmatrix, flat, preferred_element_type=jnp.float32).reshape(zfield.shape)


def reference(field, ens, sdev, lon_taper, static_taper, loc_vert, static_vert, obs_block, obs_value, obs_rinv, obs_horiz, obs_vert):
    def member(total, pert):
        zpert = (pert.astype(jnp.float32) * field).astype(jnp.bfloat16)
        return total + pert.astype(jnp.float32) * localize(zpert, lon_taper, loc_vert), None

    ens_sum, _ = lax.scan(member, jnp.zeros(field.shape, jnp.float32), ens)
    spart = (sdev * field).astype(jnp.bfloat16)
    static_sum = localize(spart, static_taper, static_vert)
    increment = ens_weight * ens_sum + static_weight * sdev * static_sum
    nblk = (NLON // 8) * (LAT // 16)
    blocks = increment.reshape(LEV, NLON // 8, 8, LAT // 16, 16).transpose(0, 1, 3, 2, 4).reshape(LEV, nblk, 128)
    groups = NOBS // OBS_DEV
    ids = obs_block.reshape(groups, OBS_DEV)
    values = obs_value.reshape(groups, OBS_DEV)
    rinv = obs_rinv.reshape(groups, OBS_DEV)
    horiz = obs_horiz.reshape(groups, OBS_DEV, 128)
    vert = obs_vert.reshape(groups, OBS_DEV, LEV)

    def observe(carry, items):
        block_ids, value, weight, hpart, vpart = items
        live = block_ids >= 0
        safe = jnp.where(live, block_ids, 0).astype(jnp.int32)
        picked = jnp.take(blocks, safe, axis=1)
        hz = jnp.einsum('ljc,jc->lj', picked, hpart, precision=lax.Precision.HIGHEST)
        hx = jnp.einsum('jl,lj->j', vpart, hz, precision=lax.Precision.HIGHEST)
        miss = hx - value
        dep = jnp.where(live, weight * miss, 0.0)
        cost = 0.5 * jnp.sum(dep * miss)
        terms = (dep[:, None, None] * vpart[:, :, None]) * hpart[:, None, :]
        adj = jax.ops.segment_sum(terms, safe, num_segments=nblk)
        return (carry[0] + adj, carry[1] + cost), None

    init = (jnp.zeros((nblk, LEV, 128), jnp.float32), jnp.zeros((), jnp.float32))
    (adj_blocks, obs_cost), _ = lax.scan(observe, init, (ids, values, rinv, horiz, vert))
    adjoint_field = adj_blocks.transpose(1, 0, 2).reshape(LEV, NLON // 8, LAT // 16, 8, 16).transpose(0, 1, 3, 2, 4).reshape(LEV, NLON, LAT)
    return increment, adjoint_field, obs_cost
```

```python
import functools

import jax
import jax.numpy as jnp
from jax import lax
from jax.experimental import pallas as pl
from jax.experimental.pallas import tpu as pltpu
from jax.sharding import PartitionSpec as P

MESH = pl.DeviceIdType.MESH
F32 = jnp.float32
BF16 = jnp.bfloat16

ens_weight = 0.8
static_weight = 0.5

COLUMNS = 16
PEERS = 8
CHUNKS = 5
PAIR = 2
OWN = CHUNKS * PAIR
LEVELS = 72
ROWS = 18
QUADS = LEVELS // 4


def iota(shape, dim):
    return lax.broadcasted_iota(jnp.int32, shape, dim)


def band(taper, out):
    row, col = iota((128, 192), 0), iota((128, 192), 1)
    at = col % 48 - (row // 32) * 8 - row % 8
    same = (row // 8) % 4 == col // 48
    total = jnp.zeros((128, 192), F32)
    for d in range(17):
        total = total + jnp.where(at == d, taper[:, d : d + 1].astype(F32), 0.0)
    out[...] = jnp.where(same, total, 0.0).astype(BF16)


def spread(matrix):
    cols = (iota((LEVELS, 576), 0) == iota((LEVELS, 576), 1) // 8).astype(BF16)
    rows = (iota((144, ROWS), 0) // 8 == iota((144, ROWS), 1)).astype(BF16)
    wide = jnp.dot(matrix.astype(BF16), cols, preferred_element_type=F32).astype(BF16)
    tall = jnp.dot(rows, wide, preferred_element_type=F32)
    keep = iota((144, 576), 0) % 8 == iota((144, 576), 1) % 8
    return jnp.where(keep, tall, 0.0).astype(BF16)


def kernel(
    ens, field, spart, sdev, loc, loc_v, svert, ltaper, staper, out,
    ens_buf, field_buf, spart_buf, loc_buf, zh_buf, band_e, band_s, vert_e, vert_s, acc, sv_buf, ret_buf,
    es_send, es_recv, ey_send, ey_recv, f_send, f_recv, fy_send, fy_recv, l_send, l_recv, r_send, r_recv,
):
    lon, q = lax.axis_index("lon"), lax.axis_index("lev")
    column, h = lon // 2, lon % 2
    zlo, core = q // 2, q % 2
    left = 2 * ((column + COLUMNS - 1) % COLUMNS) + h
    right = 2 * ((column + 1) % COLUMNS) + h

    def peer(r):
        hr = 1 - h if r & 4 else h
        zr = 1 - zlo if r & 2 else zlo
        cr = 1 - core if r & 1 else core
        return hr, 2 * zr + cr

    barrier = pltpu.get_barrier_semaphore()
    for r in range(1, PEERS):
        hr, qr = peer(r)
        pl.semaphore_signal(barrier, inc=1, device_id=(2 * column + hr, qr), device_id_type=MESH)
    for side in (left, right):
        pl.semaphore_signal(barrier, inc=1, device_id=(side, q), device_id_type=MESH)
    pl.semaphore_wait(barrier, PEERS + 1)

    def remote(src, dst, send, recv, where):
        return pltpu.make_async_remote_copy(
            src_ref=src, dst_ref=dst, send_sem=send, recv_sem=recv, device_id=where, device_id_type=MESH
        )

    def column_device(r):
        hr, qr = peer(r)
        return (2 * column + hr, qr)

    pairs = ((field, field_buf), (spart, spart_buf))

    def f_slot(n, r):
        hr, qr = peer(r)
        return pairs[n][1].at[pl.ds(ROWS * qr, ROWS), pl.ds(1 + 2 * hr, 2)]

    def f_copy(n, r):
        if r == 0:
            return pltpu.make_async_copy(pairs[n][0], f_slot(n, 0), f_recv.at[n, 0])
        return remote(pairs[n][0], f_slot(n, 0), f_send.at[n, r], f_recv.at[n, r], column_device(r))

    def f_pass(n, r):
        return remote(f_slot(n, r), f_slot(n, r), f_send.at[n, r + 1], f_recv.at[n, r + 1], column_device(1))

    def f_arrived(n, r):
        if r == 0:
            return f_copy(n, 0).wait()
        remote(f_slot(n, r), f_slot(n, r), f_send.at[n, r], f_recv.at[n, r], column_device(r)).wait_recv()

    def l_copy(r):
        return remote(loc, loc_buf.at[q], l_send.at[r], l_recv.at[r], column_device(r))

    def l_arrived(r):
        hr, qr = peer(r)
        remote(loc, loc_buf.at[qr], l_send.at[r], l_recv.at[r], column_device(r)).wait_recv()

    def e_copy(c, half, r):
        hr, qr = peer(r)
        here = h if half == 0 else 1 - h
        there = 1 + 3 * h if half == 0 else 2 + h
        src = ens.at[pl.ds(OWN * (4 * hr + qr) + PAIR * c, PAIR), :, here]
        dst = ens_buf.at[c, :, pl.ds(ROWS * q, ROWS), there]
        if r == 0:
            return pltpu.make_async_copy(src, dst, es_recv.at[c, half, 0])
        return remote(src, dst, es_send.at[c, half, r], es_recv.at[c, half, r], column_device(r))

    def e_arrived(c, half):
        e_copy(c, half, 0).wait()
        for r in range(1, PEERS):
            hr, qr = peer(r)
            there = 1 + 3 * hr if half == 0 else 2 + hr
            slot = ens_buf.at[c, :, pl.ds(ROWS * qr, ROWS), there]
            remote(slot, slot, es_send.at[c, half, r], es_recv.at[c, half, r], column_device(r)).wait_recv()

    def sides(buf, send, recv, lead):
        mine = [buf.at[lead + (slice(None), 1)], buf.at[lead + (slice(None), 4)]]
        theirs = [buf.at[lead + (slice(None), 5)], buf.at[lead + (slice(None), 0)]]
        return [
            remote(mine[s], theirs[s], send.at[s], recv.at[s], ((left, right)[s], q)) for s in range(2)
        ]

    def e_sides(c):
        return [s for k in range(PAIR) for s in sides(ens_buf, ey_send.at[c, k], ey_recv.at[c, k], (c, k))]

    def f_sides():
        return sides(field_buf, fy_send.at[0], fy_recv.at[0], ()) + sides(
            spart_buf, fy_send.at[1], fy_recv.at[1], ()
        )

    order = (4, 6, 7, 5, 2, 3, 1)
    for n in range(2):
        for r in (4, 6, 2, 1, 0):
            f_copy(n, r).start()
    for r in (2, 3, 1):
        l_copy(r).start()

    def send_members(c, half):
        for r in order:
            e_copy(c, half, r).start()
        e_copy(c, half, 0).start()

    send_members(0, 0)
    for c in range(1, CHUNKS):
        send_members(c, 0)
        send_members(c - 1, 1)
    send_members(CHUNKS - 1, 1)

    band(ltaper[...], band_e)
    band(staper[...], band_s)
    vert_s[...] = spread(svert[...])
    vert_e[pl.ds(144 * q, 144)] = spread(loc_v[...])
    for r in (1, 2, 3):
        l_arrived(r)
        hr, qr = peer(r)
        vert_e[pl.ds(144 * qr, 144)] = spread(loc_buf[qr])
    acc[...] = jnp.zeros_like(acc)

    for r in (2, 6, 4):
        for n in range(2):
            f_arrived(n, r)
            f_pass(n, r).start()
    for n in range(2):
        for r in (0, 1, 3, 5, 7):
            f_arrived(n, r)
    for s in f_sides():
        s.start()

    def smooth(weights, read):
        def quad(n, _):
            out_rows = jnp.dot(weights[...], read(4 * n), preferred_element_type=F32).astype(BF16)
            lanes = out_rows.shape[1]
            for ib in range(4):
                zh_buf[ib, pl.ds(pl.multiple_of(32 * n, 32), 32), :lanes] = out_rows[32 * ib : 32 * ib + 32]
            return 0

        lax.fori_loop(0, QUADS, quad, 0)

    def read_static(m):
        return spart_buf[pl.ds(m, 4)].astype(F32).reshape(192, 128).astype(BF16)

    def members(c):
        def read(m):
            weight = field_buf[pl.ds(m, 4)]
            both = [(ens_buf[c, k, pl.ds(m, 4)].astype(F32) * weight).reshape(192, 128) for k in range(PAIR)]
            return jnp.concatenate(both, axis=1).astype(BF16)

        smooth(band_e, read)

        def part(n, _):
            ib, third = n // 3, n % 3
            rows = pl.ds(pl.multiple_of(192 * third, 192), 192)
            levels = pl.ds(24 * third, 24)
            mixed = jnp.dot(vert_e[rows], zh_buf[ib], preferred_element_type=F32)
            total = acc[ib, levels]
            for k in range(PAIR):
                value = mixed[:, 128 * k : 128 * k + 128].reshape(24, 8, 128)
                total = total + ens_buf[c, k, levels, 1 + ib].astype(F32) * value
            acc[ib, levels] = total
            return 0

        lax.fori_loop(0, 12, part, 0)

    e_arrived(0, 0)
    for s in e_sides(0):
        s.start()
    for s in f_sides():
        s.wait()
    smooth(band_s, read_static)
    for i in range(2):
        sv = jnp.dot(vert_s[...], zh_buf[2 * h + i, :, :128], preferred_element_type=F32)
        sv_buf[i] = sv.reshape(ROWS, 8, 128)

    def chunk(c, _):
        @pl.when(c + 1 < CHUNKS)
        def _():
            e_arrived(c + 1, 0)
            for s in e_sides(c + 1):
                s.start()

        e_arrived(c, 1)
        for s in e_sides(c):
            s.wait()
        members(c)
        return 0

    lax.fori_loop(0, CHUNKS, chunk, 0)

    def r_copy(r):
        hr, qr = peer(r)
        return remote(
            acc.at[pl.ds(2 * hr, 2), pl.ds(ROWS * qr, ROWS)], ret_buf.at[r], r_send.at[r], r_recv.at[r], column_device(r)
        )

    for r in order:
        r_copy(r).start()
    for r in order:
        r_copy(r).wait_recv()
    for i in range(2):
        total = acc[2 * h + i, pl.ds(ROWS * q, ROWS)]
        for r in range(1, PEERS):
            total = total + ret_buf[r, i]
        out[:, i] = ens_weight * total + static_weight * sdev[:, i] * sv_buf[i]

    for r in range(1, PEERS):
        r_copy(r).wait_send()
    for r in (1, 2, 3):
        l_copy(r).wait_send()
    for n in range(2):
        for r in (1, 2, 4, 6):
            f_copy(n, r).wait_send()
        for r in (2, 4, 6):
            f_pass(n, r).wait_send()

    def sent(c, _):
        for half in range(2):
            for r in range(1, PEERS):
                e_copy(c, half, r).wait_send()
        return 0

    lax.fori_loop(0, CHUNKS, sent, 0)


def increment_of(field, ens, sdev, lon_taper, static_taper, loc_vert, static_vert):
    members = ens.shape[0]
    spart = (sdev * field).astype(BF16).reshape(ROWS, 2, 8, 128)
    vmem = pl.BlockSpec(memory_space=pltpu.VMEM)
    hbm = pl.BlockSpec(memory_space=pltpu.HBM)
    loc = loc_vert.astype(F32)
    dma = pltpu.SemaphoreType.DMA
    out = pl.pallas_call(
        kernel,
        out_shape=jax.ShapeDtypeStruct((ROWS, 2, 8, 128), F32),
        in_specs=[hbm, hbm, hbm, vmem, hbm, vmem, vmem, vmem, vmem],
        out_specs=vmem,
        scratch_shapes=[
            pltpu.VMEM((CHUNKS, PAIR, LEVELS, 6, 8, 128), BF16),
            pltpu.VMEM((LEVELS, 6, 8, 128), F32),
            pltpu.VMEM((LEVELS, 6, 8, 128), BF16),
            pltpu.VMEM((4, ROWS, LEVELS), F32),
            pltpu.VMEM((4, 576, 256), BF16),
            pltpu.VMEM((128, 192), BF16),
            pltpu.VMEM((128, 192), BF16),
            pltpu.VMEM((576, 576), BF16),
            pltpu.VMEM((144, 576), BF16),
            pltpu.VMEM((4, LEVELS, 8, 128), F32),
            pltpu.VMEM((2, ROWS, 8, 128), F32),
            pltpu.VMEM((PEERS, 2, ROWS, 8, 128), F32),
            dma((CHUNKS, 2, PEERS)),
            dma((CHUNKS, 2, PEERS)),
            dma((CHUNKS, PAIR, 2)),
            dma((CHUNKS, PAIR, 2)),
            dma((2, PEERS)),
            dma((2, PEERS)),
            dma((2, 2)),
            dma((2, 2)),
            dma((4,)),
            dma((4,)),
            dma((PEERS,)),
            dma((PEERS,)),
        ],
        compiler_params=pltpu.CompilerParams(
            collective_id=0, has_side_effects=True, vmem_limit_bytes=48 * 1024 * 1024
        ),
        name="members",
    )(
        ens.reshape(members, ROWS, 2, 8, 128),
        field.reshape(ROWS, 2, 8, 128),
        spart,
        sdev.reshape(ROWS, 2, 8, 128),
        loc,
        loc,
        static_vert,
        lon_taper[None],
        static_taper[None],
    )
    return out.reshape(ROWS, 16, 128)


def sent_to_all(x, axis):
    copies = jnp.broadcast_to(x, (lax.axis_size(axis), *x.shape))
    return lax.all_to_all(copies, axis, split_axis=0, concat_axis=0, tiled=True)


def taken_together(x, axis):
    return sent_to_all(x, axis).sum(axis=0)


def body(
    field,
    ens,
    sdev,
    lon_taper,
    static_taper,
    loc_vert,
    static_vert,
    obs_block,
    obs_value,
    obs_rinv,
    obs_horiz,
    obs_vert,
):
    _, lev_rows, lon_cols, lat_rows = ens.shape
    increment = increment_of(field, ens, sdev, lon_taper, static_taper, loc_vert, static_vert)
    block_lon = lon_cols // 8
    block_lat = lat_rows // 16
    nblk = block_lon * block_lat
    slots = obs_block.shape[0]
    blocks = (
        increment.reshape(lev_rows, block_lon, 8, block_lat, 16)
        .transpose(0, 1, 3, 2, 4)
        .reshape(lev_rows * nblk, 128)
    )
    live = obs_block >= 0
    local_ids = obs_block - lax.axis_index("lon") * nblk
    safe = jnp.where(live, local_ids, 0)
    selector = ((jnp.arange(nblk)[:, None] == safe[None, :]) & live[None, :]).astype(jnp.float32)
    vert_rows = obs_vert.T
    projected = jnp.dot(blocks, obs_horiz.T, precision=lax.Precision.HIGHEST).reshape(
        lev_rows, nblk, slots
    )
    picked = jnp.sum(projected * selector[None], axis=1)
    partial_value = jnp.sum(picked * vert_rows, axis=0)
    hx = taken_together(partial_value, "lev")
    miss = hx - obs_value
    dep = jnp.where(live, obs_rinv * miss, 0.0)
    obs_cost = taken_together(0.5 * jnp.sum(dep * miss), "lon")
    weights = vert_rows * dep[None, :]
    spread = (weights[:, None, :] * selector[None]).reshape(lev_rows * nblk, slots)
    adj_blocks = jnp.dot(spread, obs_horiz, precision=lax.Precision.HIGHEST)
    adjoint_field = (
        adj_blocks.reshape(lev_rows, block_lon, block_lat, 8, 16)
        .transpose(0, 1, 3, 2, 4)
        .reshape(lev_rows, lon_cols, lat_rows)
    )
    return (increment, adjoint_field, obs_cost)


def solution(mesh):
    return jax.shard_map(
        body,
        mesh=mesh,
        in_specs=(
            P("lev", "lon", None),
            P(None, "lev", "lon", None),
            P("lev", "lon", None),
            P(),
            P(),
            P("lev", None),
            P("lev", None),
            P("lon"),
            P("lon"),
            P("lon"),
            P("lon", None),
            P("lon", "lev"),
        ),
        out_specs=(P("lev", "lon", None), P("lev", "lon", None), P()),
        check_vma=False,
    )
```

```python
import functools

import jax
import jax.numpy as jnp
from jax import lax
from jax.experimental import pallas as pl
from jax.experimental.pallas import tpu as pltpu
from jax.sharding import PartitionSpec as P

MESH = pl.DeviceIdType.MESH
F32 = jnp.float32
BF16 = jnp.bfloat16

ens_weight = 0.8
static_weight = 0.5

COLUMNS = 16
PEERS = 8
CHUNKS = 5
PAIR = 2
OWN = CHUNKS * PAIR
LEVELS = 72
ROWS = 18
QUADS = LEVELS // 4


def iota(shape, dim):
    return lax.broadcasted_iota(jnp.int32, shape, dim)


def band(taper, out):
    row, col = iota((128, 192), 0), iota((128, 192), 1)
    at = col % 48 - (row // 32) * 8 - row % 8
    same = (row // 8) % 4 == col // 48
    total = jnp.zeros((128, 192), F32)
    for d in range(17):
        total = total + jnp.where(at == d, taper[:, d : d + 1].astype(F32), 0.0)
    out[...] = jnp.where(same, total, 0.0).astype(BF16)


def spread(matrix):
    cols = (iota((LEVELS, 576), 0) == iota((LEVELS, 576), 1) // 8).astype(BF16)
    rows = (iota((144, ROWS), 0) // 8 == iota((144, ROWS), 1)).astype(BF16)
    wide = jnp.dot(matrix.astype(BF16), cols, preferred_element_type=F32).astype(BF16)
    tall = jnp.dot(rows, wide, preferred_element_type=F32)
    keep = iota((144, 576), 0) % 8 == iota((144, 576), 1) % 8
    return jnp.where(keep, tall, 0.0).astype(BF16)


def swapped(x):
    row, group = iota(x.shape, 1), iota(x.shape, 2) // 16
    for b in (1, 2, 4):
        row_bit, group_bit = (row // b) % 2, (group // b) % 2
        after = pltpu.roll(pltpu.roll(x, 8 - b, 1), 16 * b, 2)
        before = after if b == 4 else pltpu.roll(pltpu.roll(x, b, 1), 128 - 16 * b, 2)
        x = jnp.where(row_bit == group_bit, x, jnp.where(row_bit == 0, after, before))
    return x


def halves(x):
    high = x.astype(BF16)
    return high, (x - high.astype(F32)).astype(BF16)


def kernel(
    ens, field, sdev, ltaper, staper, loc, svert, block, value, rinv, horiz, vert,
    inc_out, adj_out, cost_out,
    ens_buf, field_buf, spart_buf, loc_buf, zh_buf, band_e, band_s, vert_e, vert_s, acc, sv_buf,
    d_buf, r_out, r_buf,
    field_v, sdev_v, svert_v, ltaper_v, staper_v, block_v, value_v, rinv_v, horiz_v, vert_v,
    pick, h_cat, h_turned, spread_hi, spread_lo, hx_all, cost_y, cost_x, cost_h,
    es_send, es_recv, ey_send, ey_recv, f_send, f_recv, fy_send, fy_recv, l_send, l_recv,
    d_send, d_recv, r_send, r_recv, x_send, x_recv, c_send, c_recv, in_sem,
):
    lon, q = lax.axis_index("lon"), lax.axis_index("lev")
    column, h = lon // 2, lon % 2
    zlo, core = q // 2, q % 2
    px, py = lon // 8, (lon // 2) % 4
    left = 2 * ((column + COLUMNS - 1) % COLUMNS) + h
    right = 2 * ((column + 1) % COLUMNS) + h

    def peer(r):
        hr = 1 - h if r & 4 else h
        zr = 1 - zlo if r & 2 else zlo
        cr = 1 - core if r & 1 else core
        return hr, 2 * zr + cr

    def column_device(r):
        hr, qr = peer(r)
        return (2 * column + hr, qr)

    def y_device(k):
        return (8 * px + 2 * ((py + k) % 4) + h, q)

    def x_device(k):
        return (8 * ((px + k) % 4) + 2 * py + h, q)

    early = [(field, field_v), (sdev, sdev_v), (loc, loc_buf.at[q]), (svert, svert_v)]
    early += [(ltaper, ltaper_v), (staper, staper_v)]
    late = [(block, block_v), (value, value_v), (rinv, rinv_v), (horiz, horiz_v), (vert, vert_v)]
    loads = [pltpu.make_async_copy(src, dst, in_sem.at[n]) for n, (src, dst) in enumerate(early + late)]
    for copy in loads[: len(early)]:
        copy.start()

    barrier = pltpu.get_barrier_semaphore()
    greeted = [column_device(r) for r in range(1, PEERS)] + [(left, q), (right, q)]
    greeted += [y_device(k) for k in (1, 2, 3)] + [x_device(k) for k in (1, 2, 3)]
    for device in greeted:
        pl.semaphore_signal(barrier, inc=1, device_id=device, device_id_type=MESH)

    for copy in loads[: len(early)]:
        copy.wait()
    own = pl.ds(ROWS * q, ROWS)
    for i in range(2):
        spart_buf[own, 1 + 2 * h + i] = (sdev_v[:, i] * field_v[:, i]).astype(BF16)
        field_buf[own, 1 + 2 * h + i] = field_v[:, i]
    pl.semaphore_wait(barrier, len(greeted))

    def remote(src, dst, send, recv, where):
        return pltpu.make_async_remote_copy(
            src_ref=src, dst_ref=dst, send_sem=send, recv_sem=recv, device_id=where, device_id_type=MESH
        )

    bufs = (field_buf, spart_buf)

    def f_slot(n, r):
        hr, qr = peer(r)
        return bufs[n].at[pl.ds(ROWS * qr, ROWS), pl.ds(1 + 2 * hr, 2)]

    def f_copy(n, r):
        src = field_v if n == 0 else f_slot(n, 0)
        return remote(src, f_slot(n, 0), f_send.at[n, r], f_recv.at[n, r], column_device(r))

    def f_pass(n, r):
        return remote(f_slot(n, r), f_slot(n, r), f_send.at[n, r + 1], f_recv.at[n, r + 1], column_device(1))

    def f_arrived(n, r):
        remote(f_slot(n, r), f_slot(n, r), f_send.at[n, r], f_recv.at[n, r], column_device(r)).wait_recv()

    def l_copy(r):
        return remote(loc_buf.at[q], loc_buf.at[q], l_send.at[r], l_recv.at[r], column_device(r))

    def l_arrived(r):
        hr, qr = peer(r)
        remote(loc_buf.at[qr], loc_buf.at[qr], l_send.at[r], l_recv.at[r], column_device(r)).wait_recv()

    def e_copy(c, half, r):
        hr, qr = peer(r)
        here = h if half == 0 else 1 - h
        there = 1 + 3 * h if half == 0 else 2 + h
        src = ens.at[pl.ds(OWN * (4 * hr + qr) + PAIR * c, PAIR), :, here]
        dst = ens_buf.at[c, :, pl.ds(ROWS * q, ROWS), there]
        if r == 0:
            return pltpu.make_async_copy(src, dst, es_recv.at[c, half, 0])
        return remote(src, dst, es_send.at[c, half, r], es_recv.at[c, half, r], column_device(r))

    def e_arrived(c, half):
        e_copy(c, half, 0).wait()
        for r in range(1, PEERS):
            hr, qr = peer(r)
            there = 1 + 3 * hr if half == 0 else 2 + hr
            slot = ens_buf.at[c, :, pl.ds(ROWS * qr, ROWS), there]
            remote(slot, slot, es_send.at[c, half, r], es_recv.at[c, half, r], column_device(r)).wait_recv()

    def sides(buf, send, recv, lead):
        mine = [buf.at[lead + (slice(None), 1)], buf.at[lead + (slice(None), 4)]]
        theirs = [buf.at[lead + (slice(None), 5)], buf.at[lead + (slice(None), 0)]]
        return [
            remote(mine[s], theirs[s], send.at[s], recv.at[s], ((left, right)[s], q)) for s in range(2)
        ]

    def e_sides(c):
        return [s for k in range(PAIR) for s in sides(ens_buf, ey_send.at[c, k], ey_recv.at[c, k], (c, k))]

    def f_sides():
        return sides(field_buf, fy_send.at[0], fy_recv.at[0], ()) + sides(
            spart_buf, fy_send.at[1], fy_recv.at[1], ()
        )

    order = (4, 6, 7, 5, 2, 3, 1)
    for n in range(2):
        for r in (4, 6, 2, 1):
            f_copy(n, r).start()
    for r in (2, 3, 1):
        l_copy(r).start()

    def send_members(c, half):
        for r in order:
            e_copy(c, half, r).start()
        e_copy(c, half, 0).start()

    send_members(0, 0)
    for c in range(1, CHUNKS):
        send_members(c, 0)
        send_members(c - 1, 1)
    send_members(CHUNKS - 1, 1)
    for copy in loads[len(early) :]:
        copy.start()

    band(ltaper_v[...], band_e)
    band(staper_v[...], band_s)
    vert_s[...] = spread(svert_v[...])
    vert_e[pl.ds(144 * q, 144)] = spread(loc_buf[q])
    for r in (1, 2, 3):
        l_arrived(r)
        hr, qr = peer(r)
        vert_e[pl.ds(144 * qr, 144)] = spread(loc_buf[qr])
    acc[...] = jnp.zeros_like(acc)

    for n in range(2):
        for r in (2, 6, 4):
            f_arrived(n, r)
            f_pass(n, r).start()
    for n in range(2):
        for r in (1, 3, 7, 5):
            f_arrived(n, r)
    for s in f_sides():
        s.start()
    e_arrived(0, 0)
    for s in e_sides(0):
        s.start()

    for copy in loads[len(early) :]:
        copy.wait()
    slots = block_v.shape[1]
    local = block_v[...] - lon * 16
    pick[...] = ((iota((16, slots), 0) == local) & (block_v[...] >= 0)).astype(F32)
    high, low = halves(horiz_v[...])
    h_cat[:, :128] = high
    h_cat[:, 128:] = low
    high, low = halves(horiz_v[...].T)
    h_turned[:128] = high
    h_turned[128:] = low

    def smooth(weights, read):
        def quad(n, _):
            out_rows = jnp.dot(weights[...], read(4 * n), preferred_element_type=F32).astype(BF16)
            lanes = out_rows.shape[1]
            for ib in range(4):
                zh_buf[ib, pl.ds(pl.multiple_of(32 * n, 32), 32), :lanes] = out_rows[32 * ib : 32 * ib + 32]
            return 0

        lax.fori_loop(0, QUADS, quad, 0, unroll=3)

    def read_static(m):
        return spart_buf[pl.ds(m, 4)].astype(F32).reshape(192, 128).astype(BF16)

    def smooth_members(c):
        def read(m):
            weight = field_buf[pl.ds(m, 4)]
            both = [(ens_buf[c, k, pl.ds(m, 4)].astype(F32) * weight).reshape(192, 128) for k in range(PAIR)]
            return jnp.concatenate(both, axis=1).astype(BF16)

        smooth(band_e, read)

    def mix(c, ib, third):
        rows = pl.ds(pl.multiple_of(192 * third, 192), 192)
        levels = pl.ds(24 * third, 24)
        mixed = jnp.dot(vert_e[rows], zh_buf[ib], preferred_element_type=F32)
        total = acc[ib, levels]
        for k in range(PAIR):
            part = mixed[:, 128 * k : 128 * k + 128].reshape(24, 8, 128)
            total = total + ens_buf[c, k, levels, 1 + ib].astype(F32) * part
        acc[ib, levels] = total
        return 0

    for s in f_sides():
        s.wait()
    smooth(band_s, read_static)
    for i in range(2):
        sv = jnp.dot(vert_s[...], zh_buf[2 * h + i, :, :128], preferred_element_type=F32)
        sv_buf[i] = static_weight * sdev_v[:, i] * sv.reshape(ROWS, 8, 128)

    def chunk(c, _):
        e_arrived(c + 1, 0)
        for s in e_sides(c + 1):
            s.start()
        e_arrived(c, 1)
        for s in e_sides(c):
            s.wait()
        smooth_members(c)
        lax.fori_loop(0, 12, lambda n, _: mix(c, n // 3, n % 3), 0, unroll=3)
        return 0

    last = CHUNKS - 1
    lax.fori_loop(0, last, chunk, 0)

    def tile(n):
        return (2 * (1 - h) + n) % 4

    def d_copy(n, far):
        there = 2 * (1 - zlo if far else zlo) + 1 - core
        src = acc.at[tile(n), pl.ds(ROWS * there, ROWS)]
        return remote(src, d_buf.at[n, far], d_send.at[n, far], d_recv.at[n, far], column_device(1))

    def r_copy(slot, i):
        src = r_out.at[(0, 0, 1)[slot], (0, 1, 1)[slot], i]
        return remote(src, r_buf.at[slot, i], r_send.at[slot, i], r_recv.at[slot, i], column_device((4, 6, 2)[slot]))

    def reduce(n):
        for far in range(2):
            d_copy(n, far).wait_recv()
        for far in range(2):
            if n >= 2 and far == 0:
                continue
            rows = pl.ds(ROWS * (2 * (1 - zlo if far else zlo) + core), ROWS)
            r_out[n // 2, far, n % 2] = (acc[tile(n), rows] + d_buf[n, far]).astype(BF16)
        for slot in (0, 1) if n < 2 else (2,):
            r_copy(slot, n % 2).start()

    e_arrived(last, 1)
    for s in e_sides(last):
        s.wait()
    smooth_members(last)
    for n in range(4):
        lax.fori_loop(0, 3, lambda third, _: mix(last, tile(n), third), 0, unroll=3)
        for far in range(2):
            d_copy(n, far).start()
        if n:
            reduce(n - 1)
    reduce(3)
    for i in range(2):
        total = acc[2 * h + i, own] + d_buf[2 + i, 0]
        for slot in range(3):
            r_copy(slot, i).wait_recv()
            total = total + r_buf[slot, i].astype(F32)
        inc_out[:, i] = ens_weight * total + sv_buf[i]

    cells = swapped(inc_out[...].reshape(36, 8, 128)).reshape(288, 128)
    high, low = halves(cells)
    projected = jnp.dot(jnp.concatenate([high, high], axis=1), h_turned[...], preferred_element_type=F32)
    projected = projected + jnp.dot(low, h_turned[:128], preferred_element_type=F32)
    total = jnp.zeros((16, slots), F32)
    for l in range(ROWS):
        total = total + vert_v[l : l + 1] * projected[16 * l : 16 * l + 16]
    hx_all[q] = jnp.sum(total * pick[...], axis=0, keepdims=True)

    def x_copy(r):
        return remote(hx_all.at[q], hx_all.at[q], x_send.at[r], x_recv.at[r], column_device(r))

    for r in (2, 3, 1):
        x_copy(r).start()
    for r in (1, 2, 3):
        hr, qr = peer(r)
        remote(hx_all.at[qr], hx_all.at[qr], x_send.at[r], x_recv.at[r], column_device(r)).wait_recv()
    miss = hx_all[0] + hx_all[1] + hx_all[2] + hx_all[3] - value_v[...]
    dep = jnp.where(block_v[...] >= 0, rinv_v[...] * miss, 0.0)
    cost = jnp.sum(0.5 * dep * miss, axis=1, keepdims=True)

    def c_copy(phase, k, slot):
        buf, device = ((cost_y, y_device), (cost_x, x_device))[phase]
        return remote(buf.at[slot], buf.at[slot], c_send.at[phase, k], c_recv.at[phase, k], device(k))

    def c_start(phase):
        for k in (2, 1, 3):
            c_copy(phase, k, (py, px)[phase]).start()

    def c_arrived(phase):
        for k in (1, 2, 3):
            c_copy(phase, k, ((py, px)[phase] + 4 - k) % 4).wait_recv()

    def c_last(slot):
        return remote(cost_h.at[slot], cost_h.at[slot], c_send.at[2, 0], c_recv.at[2, 0], column_device(4))

    cost_y[py] = jnp.broadcast_to(cost, (1, 128))
    c_start(0)

    weights = dep * pick[...]
    for l in range(ROWS):
        high, low = halves(vert_v[l : l + 1] * weights)
        spread_hi[16 * l : 16 * l + 16] = high
        spread_lo[16 * l : 16 * l + 16] = low

    c_arrived(0)
    cost_x[px] = cost_y[0] + cost_y[1] + cost_y[2] + cost_y[3]
    c_start(1)

    both = jnp.dot(spread_hi[...], h_cat[...], preferred_element_type=F32)
    adjoint = both[:, :128] + both[:, 128:]
    adjoint = adjoint + jnp.dot(spread_lo[...], h_cat[:, :128], preferred_element_type=F32)
    adj_out[...] = swapped(adjoint.reshape(36, 8, 128)).reshape(ROWS, 2, 8, 128)

    c_arrived(1)
    cost_h[h] = cost_x[0] + cost_x[1] + cost_x[2] + cost_x[3]
    c_last(h).start()

    for n in range(4):
        for far in range(2):
            d_copy(n, far).wait_send()
    for slot in range(3):
        for i in range(2):
            r_copy(slot, i).wait_send()
    for r in (1, 2, 3):
        l_copy(r).wait_send()
        x_copy(r).wait_send()
    for n in range(2):
        for r in (1, 2, 4, 6):
            f_copy(n, r).wait_send()
        for r in (2, 4, 6):
            f_pass(n, r).wait_send()

    def sent(c, _):
        for half in range(2):
            for r in range(1, PEERS):
                e_copy(c, half, r).wait_send()
        return 0

    lax.fori_loop(0, CHUNKS, sent, 0)
    for phase in range(2):
        for k in (1, 2, 3):
            c_copy(phase, k, (py, px)[phase]).wait_send()
    c_last(1 - h).wait_recv()
    cost_out[...] = cost_h[0] + cost_h[1]
    c_last(h).wait_send()


def body(
    field, ens, sdev, lon_taper, static_taper, loc_vert, static_vert, obs_block, obs_value, obs_rinv, obs_horiz, obs_vert
):
    members, slots = ens.shape[0], obs_block.shape[0]
    vmem = pl.BlockSpec(memory_space=pltpu.VMEM)
    hbm = pl.BlockSpec(memory_space=pltpu.HBM)
    dma = pltpu.SemaphoreType.DMA
    tile = (ROWS, 2, 8, 128)
    increment, adjoint, cost = pl.pallas_call(
        kernel,
        out_shape=(
            jax.ShapeDtypeStruct(tile, F32),
            jax.ShapeDtypeStruct(tile, F32),
            jax.ShapeDtypeStruct((1, 128), F32),
        ),
        in_specs=[hbm] * 12,
        out_specs=(vmem, vmem, vmem),
        scratch_shapes=[
            pltpu.VMEM((CHUNKS, PAIR, LEVELS, 6, 8, 128), BF16),
            pltpu.VMEM((LEVELS, 6, 8, 128), F32),
            pltpu.VMEM((LEVELS, 6, 8, 128), BF16),
            pltpu.VMEM((4, ROWS, LEVELS), BF16),
            pltpu.VMEM((4, 576, 256), BF16),
            pltpu.VMEM((128, 192), BF16),
            pltpu.VMEM((128, 192), BF16),
            pltpu.VMEM((576, 576), BF16),
            pltpu.VMEM((144, 576), BF16),
            pltpu.VMEM((4, LEVELS, 8, 128), F32),
            pltpu.VMEM((2, ROWS, 8, 128), F32),
            pltpu.VMEM((4, 2, ROWS, 8, 128), F32),
            pltpu.VMEM((2, 2, 2, ROWS, 8, 128), BF16),
            pltpu.VMEM((3, 2, ROWS, 8, 128), BF16),
            pltpu.VMEM(tile, F32),
            pltpu.VMEM(tile, F32),
            pltpu.VMEM((ROWS, LEVELS), BF16),
            pltpu.VMEM((1, 17), BF16),
            pltpu.VMEM((1, 17), BF16),
            pltpu.VMEM((1, slots), jnp.int32),
            pltpu.VMEM((1, slots), F32),
            pltpu.VMEM((1, slots), F32),
            pltpu.VMEM((slots, 128), F32),
            pltpu.VMEM((ROWS, slots), F32),
            pltpu.VMEM((16, slots), F32),
            pltpu.VMEM((slots, 256), BF16),
            pltpu.VMEM((256, slots), BF16),
            pltpu.VMEM((288, slots), BF16),
            pltpu.VMEM((288, slots), BF16),
            pltpu.VMEM((4, 1, slots), F32),
            pltpu.VMEM((4, 1, 128), F32),
            pltpu.VMEM((4, 1, 128), F32),
            pltpu.VMEM((2, 1, 128), F32),
            dma((CHUNKS, 2, PEERS)),
            dma((CHUNKS, 2, PEERS)),
            dma((CHUNKS, PAIR, 2)),
            dma((CHUNKS, PAIR, 2)),
            dma((2, PEERS)),
            dma((2, PEERS)),
            dma((2, 2)),
            dma((2, 2)),
            dma((4,)),
            dma((4,)),
            dma((4, 2)),
            dma((4, 2)),
            dma((3, 2)),
            dma((3, 2)),
            dma((4,)),
            dma((4,)),
            dma((3, 4)),
            dma((3, 4)),
            dma((11,)),
        ],
        compiler_params=pltpu.CompilerParams(collective_id=0, has_side_effects=True),
        name="members",
    )(
        ens.reshape(members, *tile),
        field.reshape(tile),
        sdev.reshape(tile),
        lon_taper[None],
        static_taper[None],
        loc_vert,
        static_vert,
        obs_block[None],
        obs_value[None],
        obs_rinv[None],
        obs_horiz,
        obs_vert.T,
    )
    return increment.reshape(field.shape), adjoint.reshape(field.shape), cost[0, 0]


def solution(mesh):
    return jax.shard_map(
        body,
        mesh=mesh,
        in_specs=(
            P("lev", "lon", None),
            P(None, "lev", "lon", None),
            P("lev", "lon", None),
            P(),
            P(),
            P("lev", None),
            P("lev", None),
            P("lon"),
            P("lon"),
            P("lon"),
            P("lon", None),
            P("lon", "lev"),
        ),
        out_specs=(P("lev", "lon", None), P("lev", "lon", None), P()),
        check_vma=False,
    )
```

```python
import functools

import jax
import jax.numpy as jnp
from jax import lax
from jax.experimental import pallas as pl
from jax.experimental.pallas import tpu as pltpu
from jax.sharding import PartitionSpec as P

MESH = pl.DeviceIdType.MESH
F32 = jnp.float32
BF16 = jnp.bfloat16

ens_weight = 0.8
static_weight = 0.5

COLUMNS = 16
PEERS = 8
SECTORS = 32
CHUNKS = 5
PAIR = 2
OWN = CHUNKS * PAIR
LEVELS = 72
ROWS = 18
QUADS = LEVELS // 4


def iota(shape, dim):
    return lax.broadcasted_iota(jnp.int32, shape, dim)


def band(taper, out):
    row, col = iota((128, 192), 0), iota((128, 192), 1)
    at = col % 48 - (row // 32) * 8 - row % 8
    same = (row // 8) % 4 == col // 48
    total = jnp.zeros((128, 192), F32)
    for d in range(17):
        total = total + jnp.where(at == d, taper[:, d : d + 1].astype(F32), 0.0)
    out[...] = jnp.where(same, total, 0.0).astype(BF16)


def spread(matrix):
    cols = (iota((LEVELS, 576), 0) == iota((LEVELS, 576), 1) // 8).astype(BF16)
    rows = (iota((144, ROWS), 0) // 8 == iota((144, ROWS), 1)).astype(BF16)
    wide = jnp.dot(matrix.astype(BF16), cols, preferred_element_type=F32).astype(BF16)
    tall = jnp.dot(rows, wide, preferred_element_type=F32)
    keep = iota((144, 576), 0) % 8 == iota((144, 576), 1) % 8
    return jnp.where(keep, tall, 0.0).astype(BF16)


def swapped(x):
    row, group = iota(x.shape, 1), iota(x.shape, 2) // 16
    for b in (1, 2, 4):
        row_bit, group_bit = (row // b) % 2, (group // b) % 2
        after = pltpu.roll(pltpu.roll(x, 8 - b, 1), 16 * b, 2)
        before = after if b == 4 else pltpu.roll(pltpu.roll(x, b, 1), 128 - 16 * b, 2)
        x = jnp.where(row_bit == group_bit, x, jnp.where(row_bit == 0, after, before))
    return x


def halves(x):
    high = x.astype(BF16)
    return high, (x - high.astype(F32)).astype(BF16)


def kernel(
    ens, field, sdev, ltaper, staper, loc, svert, block, value, rinv, horiz, vert,
    inc_out, adj_out, cost_out,
    ens_buf, field_buf, spart_buf, loc_buf, zh_buf, band_e, band_s, vert_e, vert_s, acc, sv_buf,
    d_buf, r_out, r_buf,
    field_v, sdev_v, svert_v, ltaper_v, staper_v, block_v, value_v, rinv_v, horiz_v, vert_v,
    pick, h_cat, h_turned, spread_hi, spread_lo, hx_all, cost_all,
    es_send, es_recv, ey_send, ey_recv, f_send, f_recv, fy_send, fy_recv, l_send, l_recv,
    d_send, d_recv, r_send, r_recv, x_send, x_recv, c_send, c_recv, in_sem, known,
):
    lon, q = lax.axis_index("lon"), lax.axis_index("lev")
    column, h = lon // 2, lon % 2
    zlo, core = q // 2, q % 2
    px, py = lon // 8, (lon // 2) % 4
    left = 2 * ((column + COLUMNS - 1) % COLUMNS) + h
    right = 2 * ((column + 1) % COLUMNS) + h

    def peer(r):
        hr = 1 - h if r & 4 else h
        zr = 1 - zlo if r & 2 else zlo
        cr = 1 - core if r & 1 else core
        return hr, 2 * zr + cr

    def column_device(r):
        hr, qr = peer(r)
        return (2 * column + hr, qr)

    def y_device(k):
        return (8 * px + 2 * ((py + k) % 4) + h, q)

    def x_device(k):
        return (8 * ((px + k) % 4) + 2 * py + h, q)

    early = [(field, field_v), (sdev, sdev_v), (loc, loc_buf.at[q]), (svert, svert_v)]
    early += [(ltaper, ltaper_v), (staper, staper_v)]
    late = [(block, block_v), (value, value_v), (rinv, rinv_v), (horiz, horiz_v), (vert, vert_v)]
    loads = [pltpu.make_async_copy(src, dst, in_sem.at[n]) for n, (src, dst) in enumerate(early + late)]
    for copy in loads[: len(early)]:
        copy.start()

    barrier = pltpu.get_barrier_semaphore()
    greeted = [column_device(r) for r in range(1, PEERS)] + [(left, q), (right, q)]
    greeted += [y_device(k) for k in (1, 2, 3)] + [x_device(k) for k in (1, 2, 3)]
    for device in greeted:
        pl.semaphore_signal(barrier, inc=1, device_id=device, device_id_type=MESH)

    for copy in loads[: len(early)]:
        copy.wait()
    own = pl.ds(ROWS * q, ROWS)
    for i in range(2):
        spart_buf[own, 1 + 2 * h + i] = (sdev_v[:, i] * field_v[:, i]).astype(BF16)
        field_buf[own, 1 + 2 * h + i] = field_v[:, i]
    pl.semaphore_wait(barrier, len(greeted))

    def remote(src, dst, send, recv, where):
        return pltpu.make_async_remote_copy(
            src_ref=src, dst_ref=dst, send_sem=send, recv_sem=recv, device_id=where, device_id_type=MESH
        )

    bufs = (field_buf, spart_buf)

    def f_slot(n, r):
        hr, qr = peer(r)
        return bufs[n].at[pl.ds(ROWS * qr, ROWS), pl.ds(1 + 2 * hr, 2)]

    def f_half(n, r, i):
        hr, qr = peer(r)
        return bufs[n].at[pl.ds(ROWS * qr, ROWS), 1 + 2 * hr + i]

    def f_relay(n, r):
        half, sem, to = (0, 4, 2) if r == 6 else (1, 0, 6)
        slot = f_half(n, r, half)
        return remote(slot, slot, f_send.at[n, sem], f_recv.at[n, sem], column_device(to))

    def f_relayed(n):
        for half, sem, via in ((0, 4, 2), (1, 0, 6)):
            slot = f_half(n, 4, half)
            remote(slot, slot, f_send.at[n, sem], f_recv.at[n, sem], column_device(via)).wait_recv()

    def f_copy(n, r):
        src = field_v if n == 0 else f_slot(n, 0)
        return remote(src, f_slot(n, 0), f_send.at[n, r], f_recv.at[n, r], column_device(r))

    def f_pass(n, r):
        return remote(f_slot(n, r), f_slot(n, r), f_send.at[n, r + 1], f_recv.at[n, r + 1], column_device(1))

    def f_arrived(n, r):
        remote(f_slot(n, r), f_slot(n, r), f_send.at[n, r], f_recv.at[n, r], column_device(r)).wait_recv()

    def l_copy(r):
        return remote(loc_buf.at[q], loc_buf.at[q], l_send.at[r], l_recv.at[r], column_device(r))

    def l_arrived(r):
        hr, qr = peer(r)
        remote(loc_buf.at[qr], loc_buf.at[qr], l_send.at[r], l_recv.at[r], column_device(r)).wait_recv()

    def e_copy(c, half, r):
        hr, qr = peer(r)
        here = h if half == 0 else 1 - h
        there = 1 + 3 * h if half == 0 else 2 + h
        src = ens.at[pl.ds(OWN * (4 * hr + qr) + PAIR * c, PAIR), :, here]
        dst = ens_buf.at[c, :, pl.ds(ROWS * q, ROWS), there]
        if r == 0:
            return pltpu.make_async_copy(src, dst, es_recv.at[c, half, 0])
        return remote(src, dst, es_send.at[c, half, r], es_recv.at[c, half, r], column_device(r))

    def e_arrived(c, half):
        e_copy(c, half, 0).wait()
        for r in range(1, PEERS):
            hr, qr = peer(r)
            there = 1 + 3 * hr if half == 0 else 2 + hr
            slot = ens_buf.at[c, :, pl.ds(ROWS * qr, ROWS), there]
            remote(slot, slot, es_send.at[c, half, r], es_recv.at[c, half, r], column_device(r)).wait_recv()

    def sides(buf, send, recv, lead):
        mine = [buf.at[lead + (slice(None), 1)], buf.at[lead + (slice(None), 4)]]
        theirs = [buf.at[lead + (slice(None), 5)], buf.at[lead + (slice(None), 0)]]
        return [
            remote(mine[s], theirs[s], send.at[s], recv.at[s], ((left, right)[s], q)) for s in range(2)
        ]

    def e_sides(c):
        return [s for k in range(PAIR) for s in sides(ens_buf, ey_send.at[c, k], ey_recv.at[c, k], (c, k))]

    def f_sides():
        return sides(field_buf, fy_send.at[0], fy_recv.at[0], ()) + sides(
            spart_buf, fy_send.at[1], fy_recv.at[1], ()
        )

    order = (4, 6, 7, 5, 2, 3, 1)
    for n in range(2):
        for r in (6, 2, 1):
            f_copy(n, r).start()
    for r in (2, 3, 1):
        l_copy(r).start()

    def send_members(c, half):
        for r in order:
            e_copy(c, half, r).start()
        e_copy(c, half, 0).start()

    send_members(0, 0)
    for k in (1, 2, 3):
        pl.semaphore_signal(known.at[0], inc=1, device_id=x_device(k), device_id_type=MESH)
    for copy in loads[len(early) :]:
        copy.start()

    band(ltaper_v[...], band_e)
    band(staper_v[...], band_s)
    for n in range(2):
        for r in (6, 2):
            f_arrived(n, r)
            f_relay(n, r).start()
            f_pass(n, r).start()
    for c in range(1, CHUNKS):
        send_members(c, 0)
        send_members(c - 1, 1)
    send_members(CHUNKS - 1, 1)
    vert_s[...] = spread(svert_v[...])
    vert_e[pl.ds(144 * q, 144)] = spread(loc_buf[q])
    for r in (1, 2, 3):
        l_arrived(r)
        hr, qr = peer(r)
        vert_e[pl.ds(144 * qr, 144)] = spread(loc_buf[qr])
    acc[...] = jnp.zeros_like(acc)

    pl.semaphore_wait(known.at[0], 3)
    hr, qr = peer(4)
    pl.semaphore_signal(known.at[1], inc=1, device_id=(2 * column + hr, qr), device_id_type=MESH)
    for n in range(2):
        f_relayed(n)
        f_pass(n, 4).start()
    pl.semaphore_wait(known.at[1], 1)
    for n in range(2):
        for r in (1, 3, 7, 5):
            f_arrived(n, r)
    for s in f_sides():
        s.start()
    e_arrived(0, 0)
    for s in e_sides(0):
        s.start()

    for copy in loads[len(early) :]:
        copy.wait()
    slots = block_v.shape[1]
    local = block_v[...] - lon * 16
    pick[...] = ((iota((16, slots), 0) == local) & (block_v[...] >= 0)).astype(F32)
    high, low = halves(horiz_v[...])
    h_cat[:, :128] = high
    h_cat[:, 128:] = low
    high, low = halves(horiz_v[...].T)
    h_turned[:128] = high
    h_turned[128:] = low

    def smooth(weights, read):
        def quad(n, _):
            out_rows = jnp.dot(weights[...], read(4 * n), preferred_element_type=F32).astype(BF16)
            lanes = out_rows.shape[1]
            for ib in range(4):
                zh_buf[ib, pl.ds(pl.multiple_of(32 * n, 32), 32), :lanes] = out_rows[32 * ib : 32 * ib + 32]
            return 0

        lax.fori_loop(0, QUADS, quad, 0, unroll=3)

    def read_static(m):
        return spart_buf[pl.ds(m, 4)].astype(F32).reshape(192, 128).astype(BF16)

    def smooth_members(c):
        def read(m):
            weight = field_buf[pl.ds(m, 4)]
            both = [(ens_buf[c, k, pl.ds(m, 4)].astype(F32) * weight).reshape(192, 128) for k in range(PAIR)]
            return jnp.concatenate(both, axis=1).astype(BF16)

        smooth(band_e, read)

    def mix(c, ib, third):
        rows = pl.ds(pl.multiple_of(192 * third, 192), 192)
        levels = pl.ds(24 * third, 24)
        mixed = jnp.dot(vert_e[rows], zh_buf[ib], preferred_element_type=F32)
        total = acc[ib, levels]
        for k in range(PAIR):
            part = mixed[:, 128 * k : 128 * k + 128].reshape(24, 8, 128)
            total = total + ens_buf[c, k, levels, 1 + ib].astype(F32) * part
        acc[ib, levels] = total
        return 0

    for s in f_sides():
        s.wait()
    smooth(band_s, read_static)
    for i in range(2):
        sv = jnp.dot(vert_s[...], zh_buf[2 * h + i, :, :128], preferred_element_type=F32)
        sv_buf[i] = static_weight * sdev_v[:, i] * sv.reshape(ROWS, 8, 128)

    def chunk(c, _):
        e_arrived(c + 1, 0)
        for s in e_sides(c + 1):
            s.start()
        e_arrived(c, 1)
        for s in e_sides(c):
            s.wait()
        smooth_members(c)
        lax.fori_loop(0, 12, lambda n, _: mix(c, n // 3, n % 3), 0, unroll=3)
        return 0

    last = CHUNKS - 1
    lax.fori_loop(0, last, chunk, 0)

    def tile(n):
        return (2 * (1 - h) + n) % 4

    def d_copy(n, far):
        there = 2 * (1 - zlo if far else zlo) + 1 - core
        src = acc.at[tile(n), pl.ds(ROWS * there, ROWS)]
        return remote(src, d_buf.at[n, far], d_send.at[n, far], d_recv.at[n, far], column_device(1))

    def r_copy(slot, i):
        src = r_out.at[(0, 0, 1)[slot], (0, 1, 1)[slot], i]
        return remote(src, r_buf.at[slot, i], r_send.at[slot, i], r_recv.at[slot, i], column_device((4, 6, 2)[slot]))

    def reduce(n):
        for far in range(2):
            d_copy(n, far).wait_recv()
        for far in range(2):
            if n >= 2 and far == 0:
                continue
            rows = pl.ds(ROWS * (2 * (1 - zlo if far else zlo) + core), ROWS)
            r_out[n // 2, far, n % 2] = (acc[tile(n), rows] + d_buf[n, far]).astype(BF16)
        for slot in (0, 1) if n < 2 else (2,):
            r_copy(slot, n % 2).start()

    e_arrived(last, 1)
    for s in e_sides(last):
        s.wait()
    smooth_members(last)
    for n in range(4):
        lax.fori_loop(0, 3, lambda third, _: mix(last, tile(n), third), 0, unroll=3)
        for far in range(2):
            d_copy(n, far).start()
        if n:
            reduce(n - 1)
    reduce(3)
    for i in range(2):
        total = acc[2 * h + i, own] + d_buf[2 + i, 0]
        for slot in range(3):
            r_copy(slot, i).wait_recv()
            total = total + r_buf[slot, i].astype(F32)
        inc_out[:, i] = ens_weight * total + sv_buf[i]

    cells = swapped(inc_out[...].reshape(36, 8, 128)).reshape(288, 128)
    high, low = halves(cells)
    projected = jnp.dot(jnp.concatenate([high, high], axis=1), h_turned[...], preferred_element_type=F32)
    projected = projected + jnp.dot(low, h_turned[:128], preferred_element_type=F32)
    total = jnp.zeros((16, slots), F32)
    for l in range(ROWS):
        total = total + vert_v[l : l + 1] * projected[16 * l : 16 * l + 16]
    hx_all[q] = jnp.sum(total * pick[...], axis=0, keepdims=True)

    def x_copy(r):
        return remote(hx_all.at[q], hx_all.at[q], x_send.at[r], x_recv.at[r], column_device(r))

    for r in (2, 3, 1):
        x_copy(r).start()
    for r in (1, 2, 3):
        hr, qr = peer(r)
        remote(hx_all.at[qr], hx_all.at[qr], x_send.at[r], x_recv.at[r], column_device(r)).wait_recv()
    miss = hx_all[0] + hx_all[1] + hx_all[2] + hx_all[3] - value_v[...]
    dep = jnp.where(block_v[...] >= 0, rinv_v[...] * miss, 0.0)
    cost = jnp.sum(0.5 * dep * miss, axis=1, keepdims=True)

    def c_copy(k, slot):
        where = ((lon + k) % SECTORS, q)
        return remote(cost_all.at[slot], cost_all.at[slot], c_send.at[k], c_recv.at[k], where)

    def c_each(act):
        def one(k, _):
            act(k)
            return 0

        lax.fori_loop(1, SECTORS, one, 0)

    cost_all[lon] = jnp.broadcast_to(cost, (1, 128))
    c_each(lambda k: c_copy(k, lon).start())

    weights = dep * pick[...]
    for l in range(ROWS):
        high, low = halves(vert_v[l : l + 1] * weights)
        spread_hi[16 * l : 16 * l + 16] = high
        spread_lo[16 * l : 16 * l + 16] = low


    both = jnp.dot(spread_hi[...], h_cat[...], preferred_element_type=F32)
    adjoint = both[:, :128] + both[:, 128:]
    adjoint = adjoint + jnp.dot(spread_lo[...], h_cat[:, :128], preferred_element_type=F32)
    adj_out[...] = swapped(adjoint.reshape(36, 8, 128)).reshape(ROWS, 2, 8, 128)


    for n in range(4):
        for far in range(2):
            d_copy(n, far).wait_send()
    for slot in range(3):
        for i in range(2):
            r_copy(slot, i).wait_send()
    for r in (1, 2, 3):
        l_copy(r).wait_send()
        x_copy(r).wait_send()
    for n in range(2):
        for r in (1, 2, 6):
            f_copy(n, r).wait_send()
        for r in (2, 6):
            f_relay(n, r).wait_send()
        for r in (2, 4, 6):
            f_pass(n, r).wait_send()

    def sent(c, _):
        for half in range(2):
            for r in range(1, PEERS):
                e_copy(c, half, r).wait_send()
        return 0

    lax.fori_loop(0, CHUNKS, sent, 0)
    c_each(lambda k: c_copy(k, lon).wait_send())
    c_each(lambda k: c_copy(k, (lon + SECTORS - k) % SECTORS).wait_recv())
    cost_out[...] = jnp.sum(cost_all[...], axis=0)


def body(
    field, ens, sdev, lon_taper, static_taper, loc_vert, static_vert, obs_block, obs_value, obs_rinv, obs_horiz, obs_vert
):
    members, slots = ens.shape[0], obs_block.shape[0]
    vmem = pl.BlockSpec(memory_space=pltpu.VMEM)
    hbm = pl.BlockSpec(memory_space=pltpu.HBM)
    dma = pltpu.SemaphoreType.DMA
    tile = (ROWS, 2, 8, 128)
    increment, adjoint, cost = pl.pallas_call(
        kernel,
        out_shape=(
            jax.ShapeDtypeStruct(tile, F32),
            jax.ShapeDtypeStruct(tile, F32),
            jax.ShapeDtypeStruct((1, 128), F32),
        ),
        in_specs=[hbm] * 12,
        out_specs=(vmem, vmem, vmem),
        scratch_shapes=[
            pltpu.VMEM((CHUNKS, PAIR, LEVELS, 6, 8, 128), BF16),
            pltpu.VMEM((LEVELS, 6, 8, 128), F32),
            pltpu.VMEM((LEVELS, 6, 8, 128), BF16),
            pltpu.VMEM((4, ROWS, LEVELS), BF16),
            pltpu.VMEM((4, 576, 256), BF16),
            pltpu.VMEM((128, 192), BF16),
            pltpu.VMEM((128, 192), BF16),
            pltpu.VMEM((576, 576), BF16),
            pltpu.VMEM((144, 576), BF16),
            pltpu.VMEM((4, LEVELS, 8, 128), F32),
            pltpu.VMEM((2, ROWS, 8, 128), F32),
            pltpu.VMEM((4, 2, ROWS, 8, 128), F32),
            pltpu.VMEM((2, 2, 2, ROWS, 8, 128), BF16),
            pltpu.VMEM((3, 2, ROWS, 8, 128), BF16),
            pltpu.VMEM(tile, F32),
            pltpu.VMEM(tile, F32),
            pltpu.VMEM((ROWS, LEVELS), BF16),
            pltpu.VMEM((1, 17), BF16),
            pltpu.VMEM((1, 17), BF16),
            pltpu.VMEM((1, slots), jnp.int32),
            pltpu.VMEM((1, slots), F32),
            pltpu.VMEM((1, slots), F32),
            pltpu.VMEM((slots, 128), F32),
            pltpu.VMEM((ROWS, slots), F32),
            pltpu.VMEM((16, slots), F32),
            pltpu.VMEM((slots, 256), BF16),
            pltpu.VMEM((256, slots), BF16),
            pltpu.VMEM((288, slots), BF16),
            pltpu.VMEM((288, slots), BF16),
            pltpu.VMEM((4, 1, slots), F32),
            pltpu.VMEM((SECTORS, 1, 128), F32),
            dma((CHUNKS, 2, PEERS)),
            dma((CHUNKS, 2, PEERS)),
            dma((CHUNKS, PAIR, 2)),
            dma((CHUNKS, PAIR, 2)),
            dma((2, PEERS)),
            dma((2, PEERS)),
            dma((2, 2)),
            dma((2, 2)),
            dma((4,)),
            dma((4,)),
            dma((4, 2)),
            dma((4, 2)),
            dma((3, 2)),
            dma((3, 2)),
            dma((4,)),
            dma((4,)),
            dma((SECTORS,)),
            dma((SECTORS,)),
            dma((11,)),
            pltpu.SemaphoreType.REGULAR((2,)),
        ],
        compiler_params=pltpu.CompilerParams(collective_id=0, has_side_effects=True, vmem_limit_bytes=48 * 1024 * 1024),
        name="members",
    )(
        *(
            pltpu.with_memory_space_constraint(x, pltpu.HBM)
            for x in (
                ens.reshape(members, *tile),
                field.reshape(tile),
                sdev.reshape(tile),
                lon_taper[None],
                static_taper[None],
                loc_vert,
                static_vert,
                obs_block[None],
                obs_value[None],
                obs_rinv[None],
                obs_horiz,
                obs_vert.T,
            )
        )
    )
    return increment.reshape(field.shape), adjoint.reshape(field.shape), cost[0, 0]


def solution(mesh):
    return jax.shard_map(
        body,
        mesh=mesh,
        in_specs=(
            P("lev", "lon", None),
            P(None, "lev", "lon", None),
            P("lev", "lon", None),
            P(),
            P(),
            P("lev", None),
            P("lev", None),
            P("lon"),
            P("lon"),
            P("lon"),
            P("lon", None),
            P("lon", "lev"),
        ),
        out_specs=(P("lev", "lon", None), P("lev", "lon", None), P()),
        check_vma=False,
    )
```

```python
import functools

import jax
import jax.numpy as jnp
from jax import lax
from jax.experimental import pallas as pl
from jax.experimental.pallas import tpu as pltpu
from jax.sharding import PartitionSpec as P

MESH = pl.DeviceIdType.MESH
F32 = jnp.float32
BF16 = jnp.bfloat16

ens_weight = 0.8
static_weight = 0.5

COLUMNS = 16
PEERS = 8
SECTORS = 32
CHUNKS = 5
PAIR = 2
OWN = CHUNKS * PAIR
LEVELS = 72
ROWS = 18
QUADS = LEVELS // 4


def iota(shape, dim):
    return lax.broadcasted_iota(jnp.int32, shape, dim)


def band(taper, out):
    row, col = iota((128, 192), 0), iota((128, 192), 1)
    at = col % 48 - (row // 32) * 8 - row % 8
    same = (row // 8) % 4 == col // 48
    total = jnp.zeros((128, 192), F32)
    for d in range(17):
        total = total + jnp.where(at == d, taper[:, d : d + 1].astype(F32), 0.0)
    out[...] = jnp.where(same, total, 0.0).astype(BF16)


def spread(matrix):
    cols = (iota((LEVELS, 576), 0) == iota((LEVELS, 576), 1) // 8).astype(BF16)
    rows = (iota((144, ROWS), 0) // 8 == iota((144, ROWS), 1)).astype(BF16)
    wide = jnp.dot(matrix.astype(BF16), cols, preferred_element_type=F32).astype(BF16)
    tall = jnp.dot(rows, wide, preferred_element_type=F32)
    keep = iota((144, 576), 0) % 8 == iota((144, 576), 1) % 8
    return jnp.where(keep, tall, 0.0).astype(BF16)


def swapped(x):
    row, group = iota(x.shape, 1), iota(x.shape, 2) // 16
    for b in (1, 2, 4):
        row_bit, group_bit = (row // b) % 2, (group // b) % 2
        after = pltpu.roll(pltpu.roll(x, 8 - b, 1), 16 * b, 2)
        before = after if b == 4 else pltpu.roll(pltpu.roll(x, b, 1), 128 - 16 * b, 2)
        x = jnp.where(row_bit == group_bit, x, jnp.where(row_bit == 0, after, before))
    return x


def far_away(k):
    x, y, z = k // 8, (k // 2) % 4, k % 2
    return min(x, 4 - x) + min(y, 4 - y) + 2 * z


def halves(x):
    high = x.astype(BF16)
    return high, (x - high.astype(F32)).astype(BF16)


def kernel(
    ens, field, sdev, ltaper, staper, loc, svert, block, value, rinv, horiz, vert,
    inc_out, adj_out, cost_out,
    ens_buf, field_buf, spart_buf, loc_buf, zh_buf, band_e, band_s, vert_e, vert_s, acc, sv_buf,
    d_buf, r_out, r_buf,
    field_v, sdev_v, svert_v, ltaper_v, staper_v, block_v, value_v, rinv_v, horiz_v, vert_v,
    pick, h_cat, h_turned, spread_hi, spread_lo, hx_all, cost_all,
    es_send, es_recv, ey_send, ey_recv, f_send, f_recv, fy_send, fy_recv, l_send, l_recv,
    d_send, d_recv, r_send, r_recv, x_send, x_recv, c_send, c_recv, in_sem, known,
):
    lon, q = lax.axis_index("lon"), lax.axis_index("lev")
    column, h = lon // 2, lon % 2
    zlo, core = q // 2, q % 2
    px, py = lon // 8, (lon // 2) % 4
    left = 2 * ((column + COLUMNS - 1) % COLUMNS) + h
    right = 2 * ((column + 1) % COLUMNS) + h

    def peer(r):
        hr = 1 - h if r & 4 else h
        zr = 1 - zlo if r & 2 else zlo
        cr = 1 - core if r & 1 else core
        return hr, 2 * zr + cr

    def column_device(r):
        hr, qr = peer(r)
        return (2 * column + hr, qr)

    def y_device(k):
        return (8 * px + 2 * ((py + k) % 4) + h, q)

    def x_device(k):
        return (8 * ((px + k) % 4) + 2 * py + h, q)

    early = [(field, field_v), (sdev, sdev_v), (loc, loc_buf.at[q]), (svert, svert_v)]
    early += [(ltaper, ltaper_v), (staper, staper_v)]
    late = [(block, block_v), (value, value_v), (rinv, rinv_v), (horiz, horiz_v), (vert, vert_v)]
    loads = [pltpu.make_async_copy(src, dst, in_sem.at[n]) for n, (src, dst) in enumerate(early + late)]
    for copy in loads[: len(early)]:
        copy.start()

    barrier = pltpu.get_barrier_semaphore()
    greeted = [column_device(r) for r in range(1, PEERS)] + [(left, q), (right, q)]
    greeted += [y_device(k) for k in (1, 2, 3)] + [x_device(k) for k in (1, 2, 3)]
    for device in greeted:
        pl.semaphore_signal(barrier, inc=1, device_id=device, device_id_type=MESH)

    for copy in loads[: len(early)]:
        copy.wait()
    own = pl.ds(ROWS * q, ROWS)
    for i in range(2):
        spart_buf[own, 1 + 2 * h + i] = (sdev_v[:, i] * field_v[:, i]).astype(BF16)
        field_buf[own, 1 + 2 * h + i] = field_v[:, i]
    pl.semaphore_wait(barrier, len(greeted))

    def remote(src, dst, send, recv, where):
        return pltpu.make_async_remote_copy(
            src_ref=src, dst_ref=dst, send_sem=send, recv_sem=recv, device_id=where, device_id_type=MESH
        )

    bufs = (field_buf, spart_buf)

    def f_slot(n, r):
        hr, qr = peer(r)
        return bufs[n].at[pl.ds(ROWS * qr, ROWS), pl.ds(1 + 2 * hr, 2)]

    def f_half(n, r, i):
        hr, qr = peer(r)
        return bufs[n].at[pl.ds(ROWS * qr, ROWS), 1 + 2 * hr + i]

    def f_relay(n, r):
        half, sem, to = (0, 4, 2) if r == 6 else (1, 0, 6)
        slot = f_half(n, r, half)
        return remote(slot, slot, f_send.at[n, sem], f_recv.at[n, sem], column_device(to))

    def f_relayed(n):
        for half, sem, via in ((0, 4, 2), (1, 0, 6)):
            slot = f_half(n, 4, half)
            remote(slot, slot, f_send.at[n, sem], f_recv.at[n, sem], column_device(via)).wait_recv()

    def f_copy(n, r):
        src = field_v if n == 0 else f_slot(n, 0)
        return remote(src, f_slot(n, 0), f_send.at[n, r], f_recv.at[n, r], column_device(r))

    def f_pass(n, r):
        return remote(f_slot(n, r), f_slot(n, r), f_send.at[n, r + 1], f_recv.at[n, r + 1], column_device(1))

    def f_arrived(n, r):
        remote(f_slot(n, r), f_slot(n, r), f_send.at[n, r], f_recv.at[n, r], column_device(r)).wait_recv()

    def l_copy(r):
        return remote(loc_buf.at[q], loc_buf.at[q], l_send.at[r], l_recv.at[r], column_device(r))

    def l_arrived(r):
        hr, qr = peer(r)
        remote(loc_buf.at[qr], loc_buf.at[qr], l_send.at[r], l_recv.at[r], column_device(r)).wait_recv()

    def piece(n, half):
        if isinstance(n, int) and half == 1 and n >= CHUNKS - 1:
            return OWN - 2 + n - (CHUNKS - 1), 1
        return PAIR * n, PAIR

    def e_copy(n, half, r):
        hr, qr = peer(r)
        first, count = piece(n, half)
        here = h if half == 0 else 1 - h
        there = 1 + 3 * h if half == 0 else 2 + h
        src = ens.at[pl.ds(OWN * (4 * hr + qr) + first, count), :, here]
        dst = ens_buf.at[pl.ds(first, count), pl.ds(ROWS * q, ROWS), there]
        if r == 0:
            return pltpu.make_async_copy(src, dst, es_recv.at[n, half, 0])
        return remote(src, dst, es_send.at[n, half, r], es_recv.at[n, half, r], column_device(r))

    def e_arrived(n, half):
        first, count = piece(n, half)
        e_copy(n, half, 0).wait()
        for r in range(1, PEERS):
            hr, qr = peer(r)
            there = 1 + 3 * hr if half == 0 else 2 + hr
            slot = ens_buf.at[pl.ds(first, count), pl.ds(ROWS * qr, ROWS), there]
            remote(slot, slot, es_send.at[n, half, r], es_recv.at[n, half, r], column_device(r)).wait_recv()

    def sides(buf, send, recv, lead):
        mine = [buf.at[lead + (slice(None), 1)], buf.at[lead + (slice(None), 4)]]
        theirs = [buf.at[lead + (slice(None), 5)], buf.at[lead + (slice(None), 0)]]
        return [
            remote(mine[s], theirs[s], send.at[s], recv.at[s], ((left, right)[s], q)) for s in range(2)
        ]

    def e_sides(c):
        return [s for k in range(PAIR) for s in sides(ens_buf, ey_send.at[c, k], ey_recv.at[c, k], (PAIR * c + k,))]

    def f_sides():
        return sides(field_buf, fy_send.at[0], fy_recv.at[0], ()) + sides(
            spart_buf, fy_send.at[1], fy_recv.at[1], ()
        )

    order = (4, 6, 7, 5, 2, 3, 1)
    for n in range(2):
        for r in (6, 2, 1):
            f_copy(n, r).start()
    for r in (2, 3, 1):
        l_copy(r).start()

    def send_members(c, half):
        for r in order:
            e_copy(c, half, r).start()
        e_copy(c, half, 0).start()

    send_members(0, 0)
    for k in (1, 2, 3):
        pl.semaphore_signal(known.at[0], inc=1, device_id=x_device(k), device_id_type=MESH)
    for copy in loads[len(early) :]:
        copy.start()

    band(ltaper_v[...], band_e)
    band(staper_v[...], band_s)
    for n in range(2):
        for r in (6, 2):
            f_arrived(n, r)
            f_relay(n, r).start()
            f_pass(n, r).start()
    for c in range(1, CHUNKS):
        send_members(c, 0)
        send_members(c - 1, 1)
    send_members(CHUNKS - 1, 1)
    send_members(CHUNKS, 1)
    vert_s[...] = spread(svert_v[...])
    vert_e[pl.ds(144 * q, 144)] = spread(loc_buf[q])
    for r in (1, 2, 3):
        l_arrived(r)
        hr, qr = peer(r)
        vert_e[pl.ds(144 * qr, 144)] = spread(loc_buf[qr])
    acc[...] = jnp.zeros_like(acc)

    pl.semaphore_wait(known.at[0], 3)
    hr, qr = peer(4)
    pl.semaphore_signal(known.at[1], inc=1, device_id=(2 * column + hr, qr), device_id_type=MESH)
    for n in range(2):
        f_relayed(n)
        f_pass(n, 4).start()
    pl.semaphore_wait(known.at[1], 1)
    for n in range(2):
        for r in (1, 3, 7, 5):
            f_arrived(n, r)
    for s in f_sides():
        s.start()
    e_arrived(0, 0)
    for s in e_sides(0):
        s.start()

    for copy in loads[len(early) :]:
        copy.wait()
    slots = block_v.shape[1]
    local = block_v[...] - lon * 16
    pick[...] = ((iota((16, slots), 0) == local) & (block_v[...] >= 0)).astype(F32)
    high, low = halves(horiz_v[...])
    h_cat[:, :128] = high
    h_cat[:, 128:] = low
    high, low = halves(horiz_v[...].T)
    h_turned[:128] = high
    h_turned[128:] = low

    def smooth(weights, read):
        def quad(n, _):
            out_rows = jnp.dot(weights[...], read(4 * n), preferred_element_type=F32).astype(BF16)
            lanes = out_rows.shape[1]
            for ib in range(4):
                zh_buf[ib, pl.ds(pl.multiple_of(32 * n, 32), 32), :lanes] = out_rows[32 * ib : 32 * ib + 32]
            return 0

        lax.fori_loop(0, QUADS, quad, 0, unroll=3)

    def read_static(m):
        return spart_buf[pl.ds(m, 4)].astype(F32).reshape(192, 128).astype(BF16)

    def smooth_members(c):
        def read(m):
            weight = field_buf[pl.ds(m, 4)]
            both = [(ens_buf[PAIR * c + k, pl.ds(m, 4)].astype(F32) * weight).reshape(192, 128) for k in range(PAIR)]
            return jnp.concatenate(both, axis=1).astype(BF16)

        smooth(band_e, read)

    def mix(c, ib, third):
        rows = pl.ds(pl.multiple_of(192 * third, 192), 192)
        levels = pl.ds(24 * third, 24)
        mixed = jnp.dot(vert_e[rows], zh_buf[ib], preferred_element_type=F32)
        total = acc[ib, levels]
        for k in range(PAIR):
            part = mixed[:, 128 * k : 128 * k + 128].reshape(24, 8, 128)
            total = total + ens_buf[PAIR * c + k, levels, 1 + ib].astype(F32) * part
        acc[ib, levels] = total
        return 0

    def smooth_one(k):
        def pair_of_quads(n, _):
            both = [
                (ens_buf[k, pl.ds(8 * n + 4 * g, 4)].astype(F32) * field_buf[pl.ds(8 * n + 4 * g, 4)]).reshape(192, 128)
                for g in range(2)
            ]
            rows = jnp.concatenate(both, axis=1).astype(BF16)
            out_rows = jnp.dot(band_e[...], rows, preferred_element_type=F32).astype(BF16)
            for ib in range(4):
                lanes = slice(128 * (ib % 2), 128 * (ib % 2) + 128)
                for g in range(2):
                    at = pl.ds(pl.multiple_of(64 * n + 32 * g, 32), 32)
                    zh_buf[ib // 2, at, lanes] = out_rows[32 * ib : 32 * ib + 32, 128 * g : 128 * g + 128]
            return 0

        lax.fori_loop(0, QUADS // 2, pair_of_quads, 0, unroll=3)

    def mix_one(k, side, third):
        rows = pl.ds(pl.multiple_of(192 * third, 192), 192)
        levels = pl.ds(24 * third, 24)
        mixed = jnp.dot(vert_e[rows], zh_buf[side], preferred_element_type=F32)
        for i in range(2):
            part = mixed[:, 128 * i : 128 * i + 128].reshape(24, 8, 128)
            tile_at = 2 * side + i
            acc[tile_at, levels] = acc[tile_at, levels] + ens_buf[k, levels, 1 + tile_at].astype(F32) * part
        return 0

    for s in f_sides():
        s.wait()
    smooth(band_s, read_static)
    for i in range(2):
        sv = jnp.dot(vert_s[...], zh_buf[2 * h + i, :, :128], preferred_element_type=F32)
        sv_buf[i] = static_weight * sdev_v[:, i] * sv.reshape(ROWS, 8, 128)

    def chunk(c, _):
        e_arrived(c + 1, 0)
        for s in e_sides(c + 1):
            s.start()
        e_arrived(c, 1)
        for s in e_sides(c):
            s.wait()
        smooth_members(c)
        lax.fori_loop(0, 12, lambda n, _: mix(c, n // 3, n % 3), 0, unroll=6)
        return 0

    last = CHUNKS - 1
    lax.fori_loop(0, last, chunk, 0)

    def tile(n):
        return (2 * (1 - h) + n) % 4

    def d_copy(n, far):
        there = 2 * (1 - zlo if far else zlo) + 1 - core
        src = acc.at[tile(n), pl.ds(ROWS * there, ROWS)]
        return remote(src, d_buf.at[n, far], d_send.at[n, far], d_recv.at[n, far], column_device(1))

    def r_copy(slot, i):
        src = r_out.at[(0, 0, 1)[slot], (0, 1, 1)[slot], i]
        return remote(src, r_buf.at[slot, i], r_send.at[slot, i], r_recv.at[slot, i], column_device((4, 6, 2)[slot]))

    def reduce(n):
        for far in range(2):
            d_copy(n, far).wait_recv()
        for far in range(2):
            if n >= 2 and far == 0:
                continue
            rows = pl.ds(ROWS * (2 * (1 - zlo if far else zlo) + core), ROWS)
            r_out[n // 2, far, n % 2] = (acc[tile(n), rows] + d_buf[n, far]).astype(BF16)
        for slot in (0, 1) if n < 2 else (2,):
            r_copy(slot, n % 2).start()

    e_arrived(last, 1)
    for s in e_sides(last):
        s.wait()
    smooth_one(OWN - 2)
    lax.fori_loop(0, 6, lambda n, _: mix_one(OWN - 2, n // 3, n % 3), 0, unroll=6)
    e_arrived(last + 1, 1)
    smooth_one(OWN - 1)
    for turn in range(2):
        side = 1 - h if turn == 0 else h
        lax.fori_loop(0, 3, lambda third, _: mix_one(OWN - 1, side, third), 0, unroll=3)
        for n in (2 * turn, 2 * turn + 1):
            for far in range(2):
                d_copy(n, far).start()
        if turn:
            reduce(0)
            reduce(1)
    reduce(2)
    reduce(3)
    for i in range(2):
        total = acc[2 * h + i, own] + d_buf[2 + i, 0]
        for slot in range(3):
            r_copy(slot, i).wait_recv()
            total = total + r_buf[slot, i].astype(F32)
        inc_out[:, i] = ens_weight * total + sv_buf[i]

    cells = swapped(inc_out[...].reshape(36, 8, 128)).reshape(288, 128)
    high, low = halves(cells)
    projected = jnp.dot(jnp.concatenate([high, high], axis=1), h_turned[...], preferred_element_type=F32)
    projected = projected + jnp.dot(low, h_turned[:128], preferred_element_type=F32)
    total = jnp.zeros((16, slots), F32)
    for l in range(ROWS):
        total = total + vert_v[l : l + 1] * projected[16 * l : 16 * l + 16]
    hx_all[q] = jnp.sum(total * pick[...], axis=0, keepdims=True)

    def x_copy(r):
        return remote(hx_all.at[q], hx_all.at[q], x_send.at[r], x_recv.at[r], column_device(r))

    for r in (2, 3, 1):
        x_copy(r).start()
    for r in (1, 2, 3):
        hr, qr = peer(r)
        remote(hx_all.at[qr], hx_all.at[qr], x_send.at[r], x_recv.at[r], column_device(r)).wait_recv()
    miss = hx_all[0] + hx_all[1] + hx_all[2] + hx_all[3] - value_v[...]
    dep = jnp.where(block_v[...] >= 0, rinv_v[...] * miss, 0.0)
    cost = jnp.sum(0.5 * dep * miss, axis=1, keepdims=True)

    def c_copy(k, slot):
        other = lon + k
        where = (jnp.where(other >= SECTORS, other - SECTORS, other), q)
        return remote(cost_all.at[slot], cost_all.at[slot], c_send.at[k], c_recv.at[k], where)

    def c_each(act):
        def one(k, _):
            act(k)
            return 0

        lax.fori_loop(1, SECTORS, one, 0)

    cost_all[lon] = jnp.broadcast_to(cost, (1, 128))
    for k in sorted(range(1, SECTORS), key=lambda k: -far_away(k)):
        c_copy(k, lon).start()

    weights = dep * pick[...]
    for l in range(ROWS):
        high, low = halves(vert_v[l : l + 1] * weights)
        spread_hi[16 * l : 16 * l + 16] = high
        spread_lo[16 * l : 16 * l + 16] = low


    both = jnp.dot(spread_hi[...], h_cat[...], preferred_element_type=F32)
    adjoint = both[:, :128] + both[:, 128:]
    adjoint = adjoint + jnp.dot(spread_lo[...], h_cat[:, :128], preferred_element_type=F32)
    adj_out[...] = swapped(adjoint.reshape(36, 8, 128)).reshape(ROWS, 2, 8, 128)


    for n in range(4):
        for far in range(2):
            d_copy(n, far).wait_send()
    for slot in range(3):
        for i in range(2):
            r_copy(slot, i).wait_send()
    for r in (1, 2, 3):
        l_copy(r).wait_send()
        x_copy(r).wait_send()
    for n in range(2):
        for r in (1, 2, 6):
            f_copy(n, r).wait_send()
        for r in (2, 6):
            f_relay(n, r).wait_send()
        for r in (2, 4, 6):
            f_pass(n, r).wait_send()

    def sent(c, _):
        for half in range(2):
            for r in range(1, PEERS):
                e_copy(c, half, r).wait_send()
        return 0

    lax.fori_loop(0, CHUNKS - 1, sent, 0)
    for r in range(1, PEERS):
        e_copy(CHUNKS - 1, 0, r).wait_send()
        e_copy(CHUNKS - 1, 1, r).wait_send()
        e_copy(CHUNKS, 1, r).wait_send()
    c_each(lambda k: c_copy(k, lon).wait_send())
    c_each(lambda k: c_copy(k, (lon + SECTORS - k) % SECTORS).wait_recv())
    cost_out[...] = jnp.sum(cost_all[...], axis=0)


def deliver(inc, adj, cost, inc_out, adj_out, cost_out, sem):
    copies = [
        pltpu.make_async_copy(src, dst, sem.at[n])
        for n, (src, dst) in enumerate(((inc, inc_out), (adj, adj_out), (cost, cost_out)))
    ]
    for copy in copies:
        copy.start()
    for copy in copies:
        copy.wait()


def body(
    field, ens, sdev, lon_taper, static_taper, loc_vert, static_vert, obs_block, obs_value, obs_rinv, obs_horiz, obs_vert
):
    members, slots = ens.shape[0], obs_block.shape[0]
    vmem = pl.BlockSpec(memory_space=pltpu.VMEM)
    hbm = pl.BlockSpec(memory_space=pltpu.HBM)
    dma = pltpu.SemaphoreType.DMA
    tile = (ROWS, 2, 8, 128)
    increment, adjoint, cost = pl.pallas_call(
        kernel,
        out_shape=(
            jax.ShapeDtypeStruct(tile, F32),
            jax.ShapeDtypeStruct(tile, F32),
            jax.ShapeDtypeStruct((1, 128), F32),
        ),
        in_specs=[hbm] * 12,
        out_specs=(vmem, vmem, vmem),
        scratch_shapes=[
            pltpu.VMEM((OWN, LEVELS, 6, 8, 128), BF16),
            pltpu.VMEM((LEVELS, 6, 8, 128), F32),
            pltpu.VMEM((LEVELS, 6, 8, 128), BF16),
            pltpu.VMEM((4, ROWS, LEVELS), BF16),
            pltpu.VMEM((4, 576, 256), BF16),
            pltpu.VMEM((128, 192), BF16),
            pltpu.VMEM((128, 192), BF16),
            pltpu.VMEM((576, 576), BF16),
            pltpu.VMEM((144, 576), BF16),
            pltpu.VMEM((4, LEVELS, 8, 128), F32),
            pltpu.VMEM((2, ROWS, 8, 128), F32),
            pltpu.VMEM((4, 2, ROWS, 8, 128), F32),
            pltpu.VMEM((2, 2, 2, ROWS, 8, 128), BF16),
            pltpu.VMEM((3, 2, ROWS, 8, 128), BF16),
            pltpu.VMEM(tile, F32),
            pltpu.VMEM(tile, F32),
            pltpu.VMEM((ROWS, LEVELS), BF16),
            pltpu.VMEM((1, 17), BF16),
            pltpu.VMEM((1, 17), BF16),
            pltpu.VMEM((1, slots), jnp.int32),
            pltpu.VMEM((1, slots), F32),
            pltpu.VMEM((1, slots), F32),
            pltpu.VMEM((slots, 128), F32),
            pltpu.VMEM((ROWS, slots), F32),
            pltpu.VMEM((16, slots), F32),
            pltpu.VMEM((slots, 256), BF16),
            pltpu.VMEM((256, slots), BF16),
            pltpu.VMEM((288, slots), BF16),
            pltpu.VMEM((288, slots), BF16),
            pltpu.VMEM((4, 1, slots), F32),
            pltpu.VMEM((SECTORS, 1, 128), F32),
            dma((CHUNKS + 1, 2, PEERS)),
            dma((CHUNKS + 1, 2, PEERS)),
            dma((CHUNKS, PAIR, 2)),
            dma((CHUNKS, PAIR, 2)),
            dma((2, PEERS)),
            dma((2, PEERS)),
            dma((2, 2)),
            dma((2, 2)),
            dma((4,)),
            dma((4,)),
            dma((4, 2)),
            dma((4, 2)),
            dma((3, 2)),
            dma((3, 2)),
            dma((4,)),
            dma((4,)),
            dma((SECTORS,)),
            dma((SECTORS,)),
            dma((11,)),
            pltpu.SemaphoreType.REGULAR((2,)),
        ],
        compiler_params=pltpu.CompilerParams(collective_id=0, has_side_effects=True, vmem_limit_bytes=48 * 1024 * 1024),
        name="members",
    )(
        *(
            pltpu.with_memory_space_constraint(x, pltpu.HBM)
            for x in (
                ens.reshape(members, *tile),
                field.reshape(tile),
                sdev.reshape(tile),
                lon_taper[None],
                static_taper[None],
                loc_vert,
                static_vert,
                obs_block[None],
                obs_value[None],
                obs_rinv[None],
                obs_horiz,
                obs_vert.T,
            )
        )
    )
    shapes = [jax.ShapeDtypeStruct(x.shape, F32) for x in (increment, adjoint, cost)]
    increment, adjoint, cost = pl.pallas_call(
        deliver,
        out_shape=shapes,
        in_specs=[vmem] * 3,
        out_specs=[hbm] * 3,
        scratch_shapes=[dma((3,))],
        compiler_params=pltpu.CompilerParams(vmem_limit_bytes=4 * 1024 * 1024),
        name="deliver",
    )(increment, adjoint, cost)
    return increment.reshape(field.shape), adjoint.reshape(field.shape), cost[0, 0]


def solution(mesh):
    return jax.shard_map(
        body,
        mesh=mesh,
        in_specs=(
            P("lev", "lon", None),
            P(None, "lev", "lon", None),
            P("lev", "lon", None),
            P(),
            P(),
            P("lev", None),
            P("lev", None),
            P("lon"),
            P("lon"),
            P("lon"),
            P("lon", None),
            P("lon", "lev"),
        ),
        out_specs=(P("lev", "lon", None), P("lev", "lon", None), P()),
        check_vma=False,
    )
```

```python
import functools

import jax
import jax.numpy as jnp
from jax import lax
from jax.experimental import pallas as pl
from jax.experimental.pallas import tpu as pltpu
from jax.sharding import PartitionSpec as P

MESH = pl.DeviceIdType.MESH
F32 = jnp.float32
BF16 = jnp.bfloat16

ens_weight = 0.8
static_weight = 0.5

COLUMNS = 16
PEERS = 8
SECTORS = 32
CHUNKS = 5
PAIR = 2
OWN = CHUNKS * PAIR
LEVELS = 72
ROWS = 18
QUADS = LEVELS // 4


def iota(shape, dim):
    return lax.broadcasted_iota(jnp.int32, shape, dim)


def band(taper, out):
    row, col = iota((128, 192), 0), iota((128, 192), 1)
    at = col % 48 - (row // 32) * 8 - row % 8
    same = (row // 8) % 4 == col // 48
    total = jnp.zeros((128, 192), F32)
    for d in range(17):
        total = total + jnp.where(at == d, taper[:, d : d + 1].astype(F32), 0.0)
    out[...] = jnp.where(same, total, 0.0).astype(BF16)


def spread(matrix):
    cols = (iota((LEVELS, 576), 0) == iota((LEVELS, 576), 1) // 8).astype(BF16)
    rows = (iota((144, ROWS), 0) // 8 == iota((144, ROWS), 1)).astype(BF16)
    wide = jnp.dot(matrix.astype(BF16), cols, preferred_element_type=F32).astype(BF16)
    tall = jnp.dot(rows, wide, preferred_element_type=F32)
    keep = iota((144, 576), 0) % 8 == iota((144, 576), 1) % 8
    return jnp.where(keep, tall, 0.0).astype(BF16)


def swapped(x):
    row, group = iota(x.shape, 1), iota(x.shape, 2) // 16
    for b in (1, 2, 4):
        row_bit, group_bit = (row // b) % 2, (group // b) % 2
        after = pltpu.roll(pltpu.roll(x, 8 - b, 1), 16 * b, 2)
        before = after if b == 4 else pltpu.roll(pltpu.roll(x, b, 1), 128 - 16 * b, 2)
        x = jnp.where(row_bit == group_bit, x, jnp.where(row_bit == 0, after, before))
    return x


def far_away(k):
    x, y, z = k // 8, (k // 2) % 4, k % 2
    return min(x, 4 - x) + min(y, 4 - y) + 2 * z


def halves(x):
    high = x.astype(BF16)
    return high, (x - high.astype(F32)).astype(BF16)


def kernel(
    ens, field, sdev, ltaper, staper, loc, svert, block, value, rinv, horiz, vert,
    inc_out, adj_out, cost_out,
    ens_buf, field_buf, spart_buf, loc_buf, zh_buf, band_e, band_s, vert_e, vert_s, acc, sv_buf,
    d_buf, r_out, r_buf,
    field_v, sdev_v, svert_v, ltaper_v, staper_v, block_v, value_v, rinv_v, horiz_v, vert_v,
    pick, h_cat, h_turned, spread_hi, spread_lo, hx_all, cost_all,
    es_send, es_recv, ey_send, ey_recv, f_send, f_recv, fy_send, fy_recv, l_send, l_recv,
    d_send, d_recv, r_send, r_recv, x_send, x_recv, c_send, c_recv, in_sem, known,
):
    lon, q = lax.axis_index("lon"), lax.axis_index("lev")
    column, h = lon // 2, lon % 2
    zlo, core = q // 2, q % 2
    px, py = lon // 8, (lon // 2) % 4
    left = 2 * ((column + COLUMNS - 1) % COLUMNS) + h
    right = 2 * ((column + 1) % COLUMNS) + h

    def peer(r):
        hr = 1 - h if r & 4 else h
        zr = 1 - zlo if r & 2 else zlo
        cr = 1 - core if r & 1 else core
        return hr, 2 * zr + cr

    def column_device(r):
        hr, qr = peer(r)
        return (2 * column + hr, qr)

    def y_device(k):
        return (8 * px + 2 * ((py + k) % 4) + h, q)

    def x_device(k):
        return (8 * ((px + k) % 4) + 2 * py + h, q)

    early = [(field, field_v), (sdev, sdev_v), (loc, loc_buf.at[q]), (svert, svert_v)]
    early += [(ltaper, ltaper_v), (staper, staper_v)]
    late = [(block, block_v), (value, value_v), (rinv, rinv_v), (horiz, horiz_v), (vert, vert_v)]
    loads = [pltpu.make_async_copy(src, dst, in_sem.at[n]) for n, (src, dst) in enumerate(early + late)]
    barrier = pltpu.get_barrier_semaphore()
    greeted = [column_device(r) for r in range(1, PEERS)] + [(left, q), (right, q)]
    greeted += [y_device(k) for k in (1, 2, 3)] + [x_device(k) for k in (1, 2, 3)]
    for device in greeted:
        pl.semaphore_signal(barrier, inc=1, device_id=device, device_id_type=MESH)

    for copy in loads[: len(early)]:
        copy.start()
    for copy in loads[: len(early)]:
        copy.wait()
    own = pl.ds(ROWS * q, ROWS)
    for i in range(2):
        spart_buf[own, 1 + 2 * h + i] = (sdev_v[:, i] * field_v[:, i]).astype(BF16)
        field_buf[own, 1 + 2 * h + i] = field_v[:, i]
    pl.semaphore_wait(barrier, len(greeted))

    def remote(src, dst, send, recv, where):
        return pltpu.make_async_remote_copy(
            src_ref=src, dst_ref=dst, send_sem=send, recv_sem=recv, device_id=where, device_id_type=MESH
        )

    bufs = (field_buf, spart_buf)

    def f_slot(n, r):
        hr, qr = peer(r)
        return bufs[n].at[pl.ds(ROWS * qr, ROWS), pl.ds(1 + 2 * hr, 2)]

    def f_half(n, r, i):
        hr, qr = peer(r)
        return bufs[n].at[pl.ds(ROWS * qr, ROWS), 1 + 2 * hr + i]

    def f_relay(n, r):
        half, sem, to = (0, 4, 2) if r == 6 else (1, 0, 6)
        slot = f_half(n, r, half)
        return remote(slot, slot, f_send.at[n, sem], f_recv.at[n, sem], column_device(to))

    def f_relayed(n):
        for half, sem, via in ((0, 4, 2), (1, 0, 6)):
            slot = f_half(n, 4, half)
            remote(slot, slot, f_send.at[n, sem], f_recv.at[n, sem], column_device(via)).wait_recv()

    def f_copy(n, r):
        src = field_v if n == 0 else f_slot(n, 0)
        return remote(src, f_slot(n, 0), f_send.at[n, r], f_recv.at[n, r], column_device(r))

    def f_pass(n, r):
        return remote(f_slot(n, r), f_slot(n, r), f_send.at[n, r + 1], f_recv.at[n, r + 1], column_device(1))

    def f_arrived(n, r):
        remote(f_slot(n, r), f_slot(n, r), f_send.at[n, r], f_recv.at[n, r], column_device(r)).wait_recv()

    def l_copy(r):
        return remote(loc_buf.at[q], loc_buf.at[q], l_send.at[r], l_recv.at[r], column_device(r))

    def l_arrived(r):
        hr, qr = peer(r)
        remote(loc_buf.at[qr], loc_buf.at[qr], l_send.at[r], l_recv.at[r], column_device(r)).wait_recv()

    def piece(n, half):
        if isinstance(n, int) and half == 1 and n >= CHUNKS - 1:
            return OWN - 2 + n - (CHUNKS - 1), 1
        return PAIR * n, PAIR

    def e_copy(n, half, r):
        hr, qr = peer(r)
        first, count = piece(n, half)
        here = h if half == 0 else 1 - h
        there = 1 + 3 * h if half == 0 else 2 + h
        src = ens.at[pl.ds(OWN * (4 * hr + qr) + first, count), :, here]
        dst = ens_buf.at[pl.ds(first, count), pl.ds(ROWS * q, ROWS), there]
        if r == 0:
            return pltpu.make_async_copy(src, dst, es_recv.at[n, half, 0])
        return remote(src, dst, es_send.at[n, half, r], es_recv.at[n, half, r], column_device(r))

    def e_arrived(n, half):
        first, count = piece(n, half)
        e_copy(n, half, 0).wait()
        for r in range(1, PEERS):
            hr, qr = peer(r)
            there = 1 + 3 * hr if half == 0 else 2 + hr
            slot = ens_buf.at[pl.ds(first, count), pl.ds(ROWS * qr, ROWS), there]
            remote(slot, slot, es_send.at[n, half, r], es_recv.at[n, half, r], column_device(r)).wait_recv()

    def sides(buf, send, recv, lead):
        mine = [buf.at[lead + (slice(None), 1)], buf.at[lead + (slice(None), 4)]]
        theirs = [buf.at[lead + (slice(None), 5)], buf.at[lead + (slice(None), 0)]]
        return [
            remote(mine[s], theirs[s], send.at[s], recv.at[s], ((left, right)[s], q)) for s in range(2)
        ]

    def e_sides(c):
        return [s for k in range(PAIR) for s in sides(ens_buf, ey_send.at[c, k], ey_recv.at[c, k], (PAIR * c + k,))]

    def f_sides():
        return sides(field_buf, fy_send.at[0], fy_recv.at[0], ()) + sides(
            spart_buf, fy_send.at[1], fy_recv.at[1], ()
        )

    order = (2, 6, 4, 3, 7, 5, 1)
    for n in range(2):
        for r in (6, 2, 1):
            f_copy(n, r).start()
    for r in (2, 3, 1):
        l_copy(r).start()

    def send_members(c, half):
        for r in order:
            e_copy(c, half, r).start()
        e_copy(c, half, 0).start()

    send_members(0, 0)
    for k in (1, 2, 3):
        pl.semaphore_signal(known.at[0], inc=1, device_id=x_device(k), device_id_type=MESH)
    for copy in loads[len(early) :]:
        copy.start()

    band(ltaper_v[...], band_e)
    band(staper_v[...], band_s)
    for n in range(2):
        for r in (6, 2):
            f_arrived(n, r)
            f_relay(n, r).start()
            f_pass(n, r).start()
    for c in range(1, CHUNKS):
        send_members(c, 0)
        send_members(c - 1, 1)
    send_members(CHUNKS - 1, 1)
    send_members(CHUNKS, 1)
    vert_s[...] = spread(svert_v[...])
    vert_e[pl.ds(144 * q, 144)] = spread(loc_buf[q])
    for r in (1, 2, 3):
        l_arrived(r)
        hr, qr = peer(r)
        vert_e[pl.ds(144 * qr, 144)] = spread(loc_buf[qr])
    acc[...] = jnp.zeros_like(acc)

    pl.semaphore_wait(known.at[0], 3)
    hr, qr = peer(4)
    pl.semaphore_signal(known.at[1], inc=1, device_id=(2 * column + hr, qr), device_id_type=MESH)
    for n in range(2):
        f_relayed(n)
        f_pass(n, 4).start()
    pl.semaphore_wait(known.at[1], 1)
    for n in range(2):
        for r in (1, 3, 7, 5):
            f_arrived(n, r)
    for s in f_sides():
        s.start()
    e_arrived(0, 0)
    for s in e_sides(0):
        s.start()

    for copy in loads[len(early) :]:
        copy.wait()
    slots = block_v.shape[1]
    local = block_v[...] - lon * 16
    pick[...] = ((iota((16, slots), 0) == local) & (block_v[...] >= 0)).astype(F32)
    high, low = halves(horiz_v[...])
    h_cat[:, :128] = high
    h_cat[:, 128:] = low
    high, low = halves(horiz_v[...].T)
    h_turned[:128] = high
    h_turned[128:] = low

    def smooth(weights, read):
        def quad(n, _):
            out_rows = jnp.dot(weights[...], read(4 * n), preferred_element_type=F32).astype(BF16)
            lanes = out_rows.shape[1]
            for ib in range(4):
                zh_buf[ib, pl.ds(pl.multiple_of(32 * n, 32), 32), :lanes] = out_rows[32 * ib : 32 * ib + 32]
            return 0

        lax.fori_loop(0, QUADS, quad, 0, unroll=9)

    def read_static(m):
        return spart_buf[pl.ds(m, 4)].astype(F32).reshape(192, 128).astype(BF16)

    def smooth_members(c):
        def read(m):
            weight = field_buf[pl.ds(m, 4)]
            both = [(ens_buf[PAIR * c + k, pl.ds(m, 4)].astype(F32) * weight).reshape(192, 128) for k in range(PAIR)]
            return jnp.concatenate(both, axis=1).astype(BF16)

        smooth(band_e, read)

    def mix(c, ib, third):
        rows = pl.ds(pl.multiple_of(192 * third, 192), 192)
        levels = pl.ds(24 * third, 24)
        mixed = jnp.dot(vert_e[rows], zh_buf[ib], preferred_element_type=F32)
        total = acc[ib, levels]
        for k in range(PAIR):
            part = mixed[:, 128 * k : 128 * k + 128].reshape(24, 8, 128)
            total = total + ens_buf[PAIR * c + k, levels, 1 + ib].astype(F32) * part
        acc[ib, levels] = total
        return 0

    def smooth_one(k):
        def pair_of_quads(n, _):
            both = [
                (ens_buf[k, pl.ds(8 * n + 4 * g, 4)].astype(F32) * field_buf[pl.ds(8 * n + 4 * g, 4)]).reshape(192, 128)
                for g in range(2)
            ]
            rows = jnp.concatenate(both, axis=1).astype(BF16)
            out_rows = jnp.dot(band_e[...], rows, preferred_element_type=F32).astype(BF16)
            for ib in range(4):
                lanes = slice(128 * (ib % 2), 128 * (ib % 2) + 128)
                for g in range(2):
                    at = pl.ds(pl.multiple_of(64 * n + 32 * g, 32), 32)
                    zh_buf[ib // 2, at, lanes] = out_rows[32 * ib : 32 * ib + 32, 128 * g : 128 * g + 128]
            return 0

        lax.fori_loop(0, QUADS // 2, pair_of_quads, 0, unroll=9)

    def mix_one(k, side, third):
        rows = pl.ds(pl.multiple_of(192 * third, 192), 192)
        levels = pl.ds(24 * third, 24)
        mixed = jnp.dot(vert_e[rows], zh_buf[side], preferred_element_type=F32)
        for i in range(2):
            part = mixed[:, 128 * i : 128 * i + 128].reshape(24, 8, 128)
            tile_at = 2 * side + i
            acc[tile_at, levels] = acc[tile_at, levels] + ens_buf[k, levels, 1 + tile_at].astype(F32) * part
        return 0

    for s in f_sides():
        s.wait()
    smooth(band_s, read_static)
    for i in range(2):
        sv = jnp.dot(vert_s[...], zh_buf[2 * h + i, :, :128], preferred_element_type=F32)
        sv_buf[i] = static_weight * sdev_v[:, i] * sv.reshape(ROWS, 8, 128)

    def chunk(c, _):
        e_arrived(c + 1, 0)
        for s in e_sides(c + 1):
            s.start()
        e_arrived(c, 1)
        for s in e_sides(c):
            s.wait()
        smooth_members(c)
        lax.fori_loop(0, 12, lambda n, _: mix(c, n // 3, n % 3), 0, unroll=12)
        return 0

    last = CHUNKS - 1
    lax.fori_loop(0, last, chunk, 0)

    def tile(n):
        return (2 * (1 - h) + n) % 4

    def d_copy(n, far):
        there = 2 * (1 - zlo if far else zlo) + 1 - core
        src = acc.at[tile(n), pl.ds(ROWS * there, ROWS)]
        return remote(src, d_buf.at[n, far], d_send.at[n, far], d_recv.at[n, far], column_device(1))

    def r_copy(slot, i):
        src = r_out.at[(0, 0, 1)[slot], (0, 1, 1)[slot], i]
        return remote(src, r_buf.at[slot, i], r_send.at[slot, i], r_recv.at[slot, i], column_device((4, 6, 2)[slot]))

    def reduce(n):
        for far in range(2):
            d_copy(n, far).wait_recv()
        for far in range(2):
            if n >= 2 and far == 0:
                continue
            rows = pl.ds(ROWS * (2 * (1 - zlo if far else zlo) + core), ROWS)
            r_out[n // 2, far, n % 2] = (acc[tile(n), rows] + d_buf[n, far]).astype(BF16)
        for slot in (0, 1) if n < 2 else (2,):
            r_copy(slot, n % 2).start()

    e_arrived(last, 1)
    for s in e_sides(last):
        s.wait()
    smooth_one(OWN - 2)
    lax.fori_loop(0, 6, lambda n, _: mix_one(OWN - 2, n // 3, n % 3), 0, unroll=6)
    e_arrived(last + 1, 1)
    smooth_one(OWN - 1)
    for turn in range(2):
        side = 1 - h if turn == 0 else h
        lax.fori_loop(0, 3, lambda third, _: mix_one(OWN - 1, side, third), 0, unroll=3)
        for n in (2 * turn, 2 * turn + 1):
            for far in range(2):
                d_copy(n, far).start()
        if turn:
            reduce(0)
            reduce(1)
    reduce(2)
    reduce(3)
    for i in range(2):
        total = acc[2 * h + i, own] + d_buf[2 + i, 0]
        for slot in range(3):
            r_copy(slot, i).wait_recv()
            total = total + r_buf[slot, i].astype(F32)
        inc_out[:, i] = ens_weight * total + sv_buf[i]

    cells = swapped(inc_out[...].reshape(36, 8, 128)).reshape(288, 128)
    high, low = halves(cells)
    projected = jnp.dot(jnp.concatenate([high, high], axis=1), h_turned[...], preferred_element_type=F32)
    projected = projected + jnp.dot(low, h_turned[:128], preferred_element_type=F32)
    total = jnp.zeros((16, slots), F32)
    for l in range(ROWS):
        total = total + vert_v[l : l + 1] * projected[16 * l : 16 * l + 16]
    hx_all[q] = jnp.sum(total * pick[...], axis=0, keepdims=True)

    def x_copy(r):
        return remote(hx_all.at[q], hx_all.at[q], x_send.at[r], x_recv.at[r], column_device(r))

    for r in (2, 3, 1):
        x_copy(r).start()
    for r in (1, 2, 3):
        hr, qr = peer(r)
        remote(hx_all.at[qr], hx_all.at[qr], x_send.at[r], x_recv.at[r], column_device(r)).wait_recv()
    miss = hx_all[0] + hx_all[1] + hx_all[2] + hx_all[3] - value_v[...]
    dep = jnp.where(block_v[...] >= 0, rinv_v[...] * miss, 0.0)
    cost = jnp.sum(0.5 * dep * miss, axis=1, keepdims=True)

    def c_copy(k, slot):
        other = lon + k
        where = (jnp.where(other >= SECTORS, other - SECTORS, other), q)
        return remote(cost_all.at[slot], cost_all.at[slot], c_send.at[k], c_recv.at[k], where)

    def c_each(act):
        def one(k, _):
            act(k)
            return 0

        lax.fori_loop(1, SECTORS, one, 0)

    cost_all[lon] = jnp.broadcast_to(cost, (1, 128))
    for k in sorted(range(1, SECTORS), key=lambda k: -far_away(k)):
        c_copy(k, lon).start()

    weights = dep * pick[...]
    for l in range(ROWS):
        high, low = halves(vert_v[l : l + 1] * weights)
        spread_hi[16 * l : 16 * l + 16] = high
        spread_lo[16 * l : 16 * l + 16] = low


    both = jnp.dot(spread_hi[...], h_cat[...], preferred_element_type=F32)
    adjoint = both[:, :128] + both[:, 128:]
    adjoint = adjoint + jnp.dot(spread_lo[...], h_cat[:, :128], preferred_element_type=F32)
    adj_out[...] = swapped(adjoint.reshape(36, 8, 128)).reshape(ROWS, 2, 8, 128)


    for n in range(4):
        for far in range(2):
            d_copy(n, far).wait_send()
    for slot in range(3):
        for i in range(2):
            r_copy(slot, i).wait_send()
    for r in (1, 2, 3):
        l_copy(r).wait_send()
        x_copy(r).wait_send()
    for n in range(2):
        for r in (1, 2, 6):
            f_copy(n, r).wait_send()
        for r in (2, 6):
            f_relay(n, r).wait_send()
        for r in (2, 4, 6):
            f_pass(n, r).wait_send()

    def sent(c, _):
        for half in range(2):
            for r in range(1, PEERS):
                e_copy(c, half, r).wait_send()
        return 0

    lax.fori_loop(0, CHUNKS - 1, sent, 0)
    for r in range(1, PEERS):
        e_copy(CHUNKS - 1, 0, r).wait_send()
        e_copy(CHUNKS - 1, 1, r).wait_send()
        e_copy(CHUNKS, 1, r).wait_send()
    c_each(lambda k: c_copy(k, lon).wait_send())
    c_each(lambda k: c_copy(k, (lon + SECTORS - k) % SECTORS).wait_recv())
    cost_out[...] = jnp.sum(cost_all[...], axis=0)


def deliver(inc, adj, cost, inc_out, adj_out, cost_out, sem):
    copies = [
        pltpu.make_async_copy(src, dst, sem.at[n])
        for n, (src, dst) in enumerate(((inc, inc_out), (adj, adj_out), (cost, cost_out)))
    ]
    for copy in copies:
        copy.start()
    for copy in copies:
        copy.wait()


def body(
    field, ens, sdev, lon_taper, static_taper, loc_vert, static_vert, obs_block, obs_value, obs_rinv, obs_horiz, obs_vert
):
    members, slots = ens.shape[0], obs_block.shape[0]
    vmem = pl.BlockSpec(memory_space=pltpu.VMEM)
    hbm = pl.BlockSpec(memory_space=pltpu.HBM)
    dma = pltpu.SemaphoreType.DMA
    tile = (ROWS, 2, 8, 128)
    increment, adjoint, cost = pl.pallas_call(
        kernel,
        out_shape=(
            jax.ShapeDtypeStruct(tile, F32),
            jax.ShapeDtypeStruct(tile, F32),
            jax.ShapeDtypeStruct((1, 128), F32),
        ),
        in_specs=[hbm] * 12,
        out_specs=(vmem, vmem, vmem),
        scratch_shapes=[
            pltpu.VMEM((OWN, LEVELS, 6, 8, 128), BF16),
            pltpu.VMEM((LEVELS, 6, 8, 128), F32),
            pltpu.VMEM((LEVELS, 6, 8, 128), BF16),
            pltpu.VMEM((4, ROWS, LEVELS), BF16),
            pltpu.VMEM((4, 576, 256), BF16),
            pltpu.VMEM((128, 192), BF16),
            pltpu.VMEM((128, 192), BF16),
            pltpu.VMEM((576, 576), BF16),
            pltpu.VMEM((144, 576), BF16),
            pltpu.VMEM((4, LEVELS, 8, 128), F32),
            pltpu.VMEM((2, ROWS, 8, 128), F32),
            pltpu.VMEM((4, 2, ROWS, 8, 128), F32),
            pltpu.VMEM((2, 2, 2, ROWS, 8, 128), BF16),
            pltpu.VMEM((3, 2, ROWS, 8, 128), BF16),
            pltpu.VMEM(tile, F32),
            pltpu.VMEM(tile, F32),
            pltpu.VMEM((ROWS, LEVELS), BF16),
            pltpu.VMEM((1, 17), BF16),
            pltpu.VMEM((1, 17), BF16),
            pltpu.VMEM((1, slots), jnp.int32),
            pltpu.VMEM((1, slots), F32),
            pltpu.VMEM((1, slots), F32),
            pltpu.VMEM((slots, 128), F32),
            pltpu.VMEM((ROWS, slots), F32),
            pltpu.VMEM((16, slots), F32),
            pltpu.VMEM((slots, 256), BF16),
            pltpu.VMEM((256, slots), BF16),
            pltpu.VMEM((288, slots), BF16),
            pltpu.VMEM((288, slots), BF16),
            pltpu.VMEM((4, 1, slots), F32),
            pltpu.VMEM((SECTORS, 1, 128), F32),
            dma((CHUNKS + 1, 2, PEERS)),
            dma((CHUNKS + 1, 2, PEERS)),
            dma((CHUNKS, PAIR, 2)),
            dma((CHUNKS, PAIR, 2)),
            dma((2, PEERS)),
            dma((2, PEERS)),
            dma((2, 2)),
            dma((2, 2)),
            dma((4,)),
            dma((4,)),
            dma((4, 2)),
            dma((4, 2)),
            dma((3, 2)),
            dma((3, 2)),
            dma((4,)),
            dma((4,)),
            dma((SECTORS,)),
            dma((SECTORS,)),
            dma((11,)),
            pltpu.SemaphoreType.REGULAR((2,)),
        ],
        compiler_params=pltpu.CompilerParams(collective_id=0, has_side_effects=True, vmem_limit_bytes=48 * 1024 * 1024),
        name="members",
    )(
        *(
            pltpu.with_memory_space_constraint(x, pltpu.HBM)
            for x in (
                ens.reshape(members, *tile),
                field.reshape(tile),
                sdev.reshape(tile),
                lon_taper[None],
                static_taper[None],
                loc_vert,
                static_vert,
                obs_block[None],
                obs_value[None],
                obs_rinv[None],
                obs_horiz,
                obs_vert.T,
            )
        )
    )
    shapes = [jax.ShapeDtypeStruct(x.shape, F32) for x in (increment, adjoint, cost)]
    increment, adjoint, cost = pl.pallas_call(
        deliver,
        out_shape=shapes,
        in_specs=[vmem] * 3,
        out_specs=[hbm] * 3,
        scratch_shapes=[dma((3,))],
        compiler_params=pltpu.CompilerParams(vmem_limit_bytes=4 * 1024 * 1024),
        name="deliver",
    )(increment, adjoint, cost)
    return increment.reshape(field.shape), adjoint.reshape(field.shape), cost[0, 0]


def solution(mesh):
    return jax.shard_map(
        body,
        mesh=mesh,
        in_specs=(
            P("lev", "lon", None),
            P(None, "lev", "lon", None),
            P("lev", "lon", None),
            P(),
            P(),
            P("lev", None),
            P("lev", None),
            P("lon"),
            P("lon"),
            P("lon"),
            P("lon", None),
            P("lon", "lev"),
        ),
        out_specs=(P("lev", "lon", None), P("lev", "lon", None), P()),
        check_vma=False,
    )
```

```python
import functools

import jax
import jax.numpy as jnp
from jax import lax
from jax.experimental import pallas as pl
from jax.experimental.pallas import tpu as pltpu
from jax.sharding import PartitionSpec as P

MESH = pl.DeviceIdType.MESH
F32 = jnp.float32
BF16 = jnp.bfloat16

ens_weight = 0.8
static_weight = 0.5

COLUMNS = 16
PEERS = 8
SECTORS = 32
GROUPS = (((0, 4), (4, 4), (8, 2)), ((0, 4), (4, 4), (8, 1), (9, 1)))
PAIR = 2
OWN = 10
LEVELS = 72
ROWS = 18
QUADS = LEVELS // 4


def iota(shape, dim):
    return lax.broadcasted_iota(jnp.int32, shape, dim)


def band(taper, out):
    row, col = iota((128, 192), 0), iota((128, 192), 1)
    at = col % 48 - (row // 32) * 8 - row % 8
    same = (row // 8) % 4 == col // 48
    total = jnp.zeros((128, 192), F32)
    for d in range(17):
        total = total + jnp.where(at == d, taper[:, d : d + 1].astype(F32), 0.0)
    out[...] = jnp.where(same, total, 0.0).astype(BF16)


def spread(matrix):
    cols = (iota((LEVELS, 576), 0) == iota((LEVELS, 576), 1) // 8).astype(BF16)
    rows = (iota((144, ROWS), 0) // 8 == iota((144, ROWS), 1)).astype(BF16)
    wide = jnp.dot(matrix.astype(BF16), cols, preferred_element_type=F32).astype(BF16)
    tall = jnp.dot(rows, wide, preferred_element_type=F32)
    keep = iota((144, 576), 0) % 8 == iota((144, 576), 1) % 8
    return jnp.where(keep, tall, 0.0).astype(BF16)


def swapped(x):
    row, group = iota(x.shape, 1), iota(x.shape, 2) // 16
    for b in (1, 2, 4):
        row_bit, group_bit = (row // b) % 2, (group // b) % 2
        after = pltpu.roll(pltpu.roll(x, 8 - b, 1), 16 * b, 2)
        before = after if b == 4 else pltpu.roll(pltpu.roll(x, b, 1), 128 - 16 * b, 2)
        x = jnp.where(row_bit == group_bit, x, jnp.where(row_bit == 0, after, before))
    return x


def far_away(k):
    x, y, z = k // 8, (k // 2) % 4, k % 2
    return min(x, 4 - x) + min(y, 4 - y) + 2 * z


def halves(x):
    high = x.astype(BF16)
    return high, (x - high.astype(F32)).astype(BF16)


def kernel(
    ens, field, sdev, ltaper, staper, loc, svert, block, value, rinv, horiz, vert,
    inc_out, adj_out, cost_out,
    ens_buf, field_buf, spart_buf, loc_buf, zh_buf, band_e, band_s, vert_e, vert_s, acc, sv_buf,
    d_buf, r_out, r_buf,
    field_v, sdev_v, svert_v, ltaper_v, staper_v, block_v, value_v, rinv_v, horiz_v, vert_v,
    pick, h_cat, h_turned, spread_hi, spread_lo, hx_all, cost_all,
    es_send, es_recv, ey_send, ey_recv, f_send, f_recv, fy_send, fy_recv, l_send, l_recv,
    d_send, d_recv, r_send, r_recv, x_send, x_recv, c_send, c_recv, in_sem, known,
):
    lon, q = lax.axis_index("lon"), lax.axis_index("lev")
    column, h = lon // 2, lon % 2
    zlo, core = q // 2, q % 2
    px, py = lon // 8, (lon // 2) % 4
    left = 2 * ((column + COLUMNS - 1) % COLUMNS) + h
    right = 2 * ((column + 1) % COLUMNS) + h

    def peer(r):
        hr = 1 - h if r & 4 else h
        zr = 1 - zlo if r & 2 else zlo
        cr = 1 - core if r & 1 else core
        return hr, 2 * zr + cr

    def column_device(r):
        hr, qr = peer(r)
        return (2 * column + hr, qr)

    def y_device(k):
        return (8 * px + 2 * ((py + k) % 4) + h, q)

    def x_device(k):
        return (8 * ((px + k) % 4) + 2 * py + h, q)

    early = [(field, field_v), (sdev, sdev_v), (loc, loc_buf.at[q]), (svert, svert_v)]
    early += [(ltaper, ltaper_v), (staper, staper_v)]
    late = [(block, block_v), (value, value_v), (rinv, rinv_v), (horiz, horiz_v), (vert, vert_v)]
    loads = [pltpu.make_async_copy(src, dst, in_sem.at[n]) for n, (src, dst) in enumerate(early + late)]
    barrier = pltpu.get_barrier_semaphore()
    greeted = [column_device(r) for r in range(1, PEERS)] + [(left, q), (right, q)]
    greeted += [y_device(k) for k in (1, 2, 3)] + [x_device(k) for k in (1, 2, 3)]
    for device in greeted:
        pl.semaphore_signal(barrier, inc=1, device_id=device, device_id_type=MESH)

    for copy in loads[: len(early)]:
        copy.start()
    for copy in loads[: len(early)]:
        copy.wait()
    own = pl.ds(ROWS * q, ROWS)
    for i in range(2):
        spart_buf[own, 1 + 2 * h + i] = (sdev_v[:, i] * field_v[:, i]).astype(BF16)
        field_buf[own, 1 + 2 * h + i] = field_v[:, i]
    pl.semaphore_wait(barrier, len(greeted))

    def remote(src, dst, send, recv, where):
        return pltpu.make_async_remote_copy(
            src_ref=src, dst_ref=dst, send_sem=send, recv_sem=recv, device_id=where, device_id_type=MESH
        )

    bufs = (field_buf, spart_buf)

    def f_slot(n, r):
        hr, qr = peer(r)
        return bufs[n].at[pl.ds(ROWS * qr, ROWS), pl.ds(1 + 2 * hr, 2)]

    def f_half(n, r, i):
        hr, qr = peer(r)
        return bufs[n].at[pl.ds(ROWS * qr, ROWS), 1 + 2 * hr + i]

    def f_relay(n, r):
        half, sem, to = (0, 4, 2) if r == 6 else (1, 0, 6)
        slot = f_half(n, r, half)
        return remote(slot, slot, f_send.at[n, sem], f_recv.at[n, sem], column_device(to))

    def f_relayed(n):
        for half, sem, via in ((0, 4, 2), (1, 0, 6)):
            slot = f_half(n, 4, half)
            remote(slot, slot, f_send.at[n, sem], f_recv.at[n, sem], column_device(via)).wait_recv()

    def f_copy(n, r):
        src = field_v if n == 0 else f_slot(n, 0)
        return remote(src, f_slot(n, 0), f_send.at[n, r], f_recv.at[n, r], column_device(r))

    def f_pass(n, r):
        return remote(f_slot(n, r), f_slot(n, r), f_send.at[n, r + 1], f_recv.at[n, r + 1], column_device(1))

    def f_arrived(n, r):
        remote(f_slot(n, r), f_slot(n, r), f_send.at[n, r], f_recv.at[n, r], column_device(r)).wait_recv()

    def l_copy(r):
        return remote(loc_buf.at[q], loc_buf.at[q], l_send.at[r], l_recv.at[r], column_device(r))

    def l_arrived(r):
        hr, qr = peer(r)
        remote(loc_buf.at[qr], loc_buf.at[qr], l_send.at[r], l_recv.at[r], column_device(r)).wait_recv()

    def e_copy(n, half, r):
        hr, qr = peer(r)
        first, count = GROUPS[half][n]
        here = h if half == 0 else 1 - h
        there = 1 + 3 * h if half == 0 else 2 + h
        src = ens.at[pl.ds(OWN * (4 * hr + qr) + first, count), :, here]
        dst = ens_buf.at[pl.ds(first, count), pl.ds(ROWS * q, ROWS), there]
        if r == 0:
            return pltpu.make_async_copy(src, dst, es_recv.at[n, half, 0])
        return remote(src, dst, es_send.at[n, half, r], es_recv.at[n, half, r], column_device(r))

    def e_arrived(n, half):
        first, count = GROUPS[half][n]
        e_copy(n, half, 0).wait()
        for r in range(1, PEERS):
            hr, qr = peer(r)
            there = 1 + 3 * hr if half == 0 else 2 + hr
            slot = ens_buf.at[pl.ds(first, count), pl.ds(ROWS * qr, ROWS), there]
            remote(slot, slot, es_send.at[n, half, r], es_recv.at[n, half, r], column_device(r)).wait_recv()

    def sides(buf, send, recv, lead):
        mine = [buf.at[lead + (slice(None), 1)], buf.at[lead + (slice(None), 4)]]
        theirs = [buf.at[lead + (slice(None), 5)], buf.at[lead + (slice(None), 0)]]
        return [
            remote(mine[s], theirs[s], send.at[s], recv.at[s], ((left, right)[s], q)) for s in range(2)
        ]

    def e_sides(c):
        first, count = GROUPS[0][c]
        members = range(first, first + count)
        return [s for k in members for s in sides(ens_buf, ey_send.at[k], ey_recv.at[k], (k,))]

    def f_sides():
        return sides(field_buf, fy_send.at[0], fy_recv.at[0], ()) + sides(
            spart_buf, fy_send.at[1], fy_recv.at[1], ()
        )

    order = (2, 6, 4, 3, 7, 5, 1)
    for n in range(2):
        for r in (6, 2, 1):
            f_copy(n, r).start()
    for r in (2, 3, 1):
        l_copy(r).start()

    def send_members(c, half):
        for r in order:
            e_copy(c, half, r).start()
        e_copy(c, half, 0).start()

    send_members(0, 0)
    for k in (1, 2, 3):
        pl.semaphore_signal(known.at[0], inc=1, device_id=x_device(k), device_id_type=MESH)
    for copy in loads[len(early) :]:
        copy.start()

    band(ltaper_v[...], band_e)
    band(staper_v[...], band_s)
    for n in range(2):
        for r in (6, 2):
            f_arrived(n, r)
            f_relay(n, r).start()
            f_pass(n, r).start()
    send_members(1, 0)
    send_members(0, 1)
    send_members(2, 0)
    for c in (1, 2, 3):
        send_members(c, 1)
    vert_s[...] = spread(svert_v[...])
    vert_e[pl.ds(144 * q, 144)] = spread(loc_buf[q])
    for r in (1, 2, 3):
        l_arrived(r)
        hr, qr = peer(r)
        vert_e[pl.ds(144 * qr, 144)] = spread(loc_buf[qr])
    acc[...] = jnp.zeros_like(acc)

    pl.semaphore_wait(known.at[0], 3)
    hr, qr = peer(4)
    pl.semaphore_signal(known.at[1], inc=1, device_id=(2 * column + hr, qr), device_id_type=MESH)
    for n in range(2):
        f_relayed(n)
        f_pass(n, 4).start()
    pl.semaphore_wait(known.at[1], 1)
    for n in range(2):
        for r in (1, 3, 7, 5):
            f_arrived(n, r)
    for s in f_sides():
        s.start()
    e_arrived(0, 0)
    for s in e_sides(0):
        s.start()

    for copy in loads[len(early) :]:
        copy.wait()
    slots = block_v.shape[1]
    local = block_v[...] - lon * 16
    pick[...] = ((iota((16, slots), 0) == local) & (block_v[...] >= 0)).astype(F32)
    high, low = halves(horiz_v[...])
    h_cat[:, :128] = high
    h_cat[:, 128:] = low
    high, low = halves(horiz_v[...].T)
    h_turned[:128] = high
    h_turned[128:] = low

    def smooth(weights, read):
        def quad(n, _):
            out_rows = jnp.dot(weights[...], read(4 * n), preferred_element_type=F32).astype(BF16)
            lanes = out_rows.shape[1]
            for ib in range(4):
                zh_buf[ib, pl.ds(pl.multiple_of(32 * n, 32), 32), :lanes] = out_rows[32 * ib : 32 * ib + 32]
            return 0

        lax.fori_loop(0, QUADS, quad, 0, unroll=9)

    def read_static(m):
        return spart_buf[pl.ds(m, 4)].astype(F32).reshape(192, 128).astype(BF16)

    def smooth_members(c):
        def read(m):
            weight = field_buf[pl.ds(m, 4)]
            both = [(ens_buf[PAIR * c + k, pl.ds(m, 4)].astype(F32) * weight).reshape(192, 128) for k in range(PAIR)]
            return jnp.concatenate(both, axis=1).astype(BF16)

        smooth(band_e, read)

    def mix(c, ib, third):
        rows = pl.ds(pl.multiple_of(192 * third, 192), 192)
        levels = pl.ds(24 * third, 24)
        mixed = jnp.dot(vert_e[rows], zh_buf[ib], preferred_element_type=F32)
        total = acc[ib, levels]
        for k in range(PAIR):
            part = mixed[:, 128 * k : 128 * k + 128].reshape(24, 8, 128)
            total = total + ens_buf[PAIR * c + k, levels, 1 + ib].astype(F32) * part
        acc[ib, levels] = total
        return 0

    def smooth_one(k):
        def pair_of_quads(n, _):
            both = [
                (ens_buf[k, pl.ds(8 * n + 4 * g, 4)].astype(F32) * field_buf[pl.ds(8 * n + 4 * g, 4)]).reshape(192, 128)
                for g in range(2)
            ]
            rows = jnp.concatenate(both, axis=1).astype(BF16)
            out_rows = jnp.dot(band_e[...], rows, preferred_element_type=F32).astype(BF16)
            for ib in range(4):
                lanes = slice(128 * (ib % 2), 128 * (ib % 2) + 128)
                for g in range(2):
                    at = pl.ds(pl.multiple_of(64 * n + 32 * g, 32), 32)
                    zh_buf[ib // 2, at, lanes] = out_rows[32 * ib : 32 * ib + 32, 128 * g : 128 * g + 128]
            return 0

        lax.fori_loop(0, QUADS // 2, pair_of_quads, 0, unroll=9)

    def mix_one(k, side, third):
        rows = pl.ds(pl.multiple_of(192 * third, 192), 192)
        levels = pl.ds(24 * third, 24)
        mixed = jnp.dot(vert_e[rows], zh_buf[side], preferred_element_type=F32)
        for i in range(2):
            part = mixed[:, 128 * i : 128 * i + 128].reshape(24, 8, 128)
            tile_at = 2 * side + i
            acc[tile_at, levels] = acc[tile_at, levels] + ens_buf[k, levels, 1 + tile_at].astype(F32) * part
        return 0

    for s in f_sides():
        s.wait()
    smooth(band_s, read_static)
    for i in range(2):
        sv = jnp.dot(vert_s[...], zh_buf[2 * h + i, :, :128], preferred_element_type=F32)
        sv_buf[i] = static_weight * sdev_v[:, i] * sv.reshape(ROWS, 8, 128)

    def pair(c, _):
        smooth_members(c)
        lax.fori_loop(0, 12, lambda n, _: mix(c, n // 3, n % 3), 0, unroll=12)
        return 0

    for g in range(2):
        e_arrived(g + 1, 0)
        for s in e_sides(g + 1):
            s.start()
        e_arrived(g, 1)
        for s in e_sides(g):
            s.wait()
        lax.fori_loop(2 * g, 2 * g + 2, pair, 0)

    def tile(n):
        return (2 * (1 - h) + n) % 4

    def d_copy(n, far):
        there = 2 * (1 - zlo if far else zlo) + 1 - core
        src = acc.at[tile(n), pl.ds(ROWS * there, ROWS)]
        return remote(src, d_buf.at[n, far], d_send.at[n, far], d_recv.at[n, far], column_device(1))

    def r_copy(slot, i):
        src = r_out.at[(0, 0, 1)[slot], (0, 1, 1)[slot], i]
        return remote(src, r_buf.at[slot, i], r_send.at[slot, i], r_recv.at[slot, i], column_device((4, 6, 2)[slot]))

    def reduce(n):
        for far in range(2):
            d_copy(n, far).wait_recv()
        for far in range(2):
            if n >= 2 and far == 0:
                continue
            rows = pl.ds(ROWS * (2 * (1 - zlo if far else zlo) + core), ROWS)
            r_out[n // 2, far, n % 2] = (acc[tile(n), rows] + d_buf[n, far]).astype(BF16)
        for slot in (0, 1) if n < 2 else (2,):
            r_copy(slot, n % 2).start()

    e_arrived(2, 1)
    for s in e_sides(2):
        s.wait()
    smooth_one(OWN - 2)
    lax.fori_loop(0, 6, lambda n, _: mix_one(OWN - 2, n // 3, n % 3), 0, unroll=6)
    e_arrived(3, 1)
    smooth_one(OWN - 1)
    for turn in range(2):
        side = 1 - h if turn == 0 else h
        lax.fori_loop(0, 3, lambda third, _: mix_one(OWN - 1, side, third), 0, unroll=3)
        for n in (2 * turn, 2 * turn + 1):
            for far in range(2):
                d_copy(n, far).start()
        if turn:
            reduce(0)
            reduce(1)
    reduce(2)
    reduce(3)
    for i in range(2):
        total = acc[2 * h + i, own] + d_buf[2 + i, 0]
        for slot in range(3):
            r_copy(slot, i).wait_recv()
            total = total + r_buf[slot, i].astype(F32)
        inc_out[:, i] = ens_weight * total + sv_buf[i]

    cells = swapped(inc_out[...].reshape(36, 8, 128)).reshape(288, 128)
    high, low = halves(cells)
    projected = jnp.dot(jnp.concatenate([high, high], axis=1), h_turned[...], preferred_element_type=F32)
    projected = projected + jnp.dot(low, h_turned[:128], preferred_element_type=F32)
    total = jnp.zeros((16, slots), F32)
    for l in range(ROWS):
        total = total + vert_v[l : l + 1] * projected[16 * l : 16 * l + 16]
    hx_all[q] = jnp.sum(total * pick[...], axis=0, keepdims=True)

    def x_copy(r):
        return remote(hx_all.at[q], hx_all.at[q], x_send.at[r], x_recv.at[r], column_device(r))

    for r in (2, 3, 1):
        x_copy(r).start()
    for r in (1, 2, 3):
        hr, qr = peer(r)
        remote(hx_all.at[qr], hx_all.at[qr], x_send.at[r], x_recv.at[r], column_device(r)).wait_recv()
    miss = hx_all[0] + hx_all[1] + hx_all[2] + hx_all[3] - value_v[...]
    dep = jnp.where(block_v[...] >= 0, rinv_v[...] * miss, 0.0)
    cost = jnp.sum(0.5 * dep * miss, axis=1, keepdims=True)

    def c_copy(k, slot):
        other = lon + k
        where = (jnp.where(other >= SECTORS, other - SECTORS, other), q)
        return remote(cost_all.at[slot], cost_all.at[slot], c_send.at[k], c_recv.at[k], where)

    def c_each(act):
        def one(k, _):
            act(k)
            return 0

        lax.fori_loop(1, SECTORS, one, 0)

    cost_all[lon] = jnp.broadcast_to(cost, (1, 128))
    for k in sorted(range(1, SECTORS), key=lambda k: -far_away(k)):
        c_copy(k, lon).start()

    weights = dep * pick[...]
    for l in range(ROWS):
        high, low = halves(vert_v[l : l + 1] * weights)
        spread_hi[16 * l : 16 * l + 16] = high
        spread_lo[16 * l : 16 * l + 16] = low


    both = jnp.dot(spread_hi[...], h_cat[...], preferred_element_type=F32)
    adjoint = both[:, :128] + both[:, 128:]
    adjoint = adjoint + jnp.dot(spread_lo[...], h_cat[:, :128], preferred_element_type=F32)
    adj_out[...] = swapped(adjoint.reshape(36, 8, 128)).reshape(ROWS, 2, 8, 128)


    for n in range(4):
        for far in range(2):
            d_copy(n, far).wait_send()
    for slot in range(3):
        for i in range(2):
            r_copy(slot, i).wait_send()
    for r in (1, 2, 3):
        l_copy(r).wait_send()
        x_copy(r).wait_send()
    for n in range(2):
        for r in (1, 2, 6):
            f_copy(n, r).wait_send()
        for r in (2, 6):
            f_relay(n, r).wait_send()
        for r in (2, 4, 6):
            f_pass(n, r).wait_send()

    for half in range(2):
        for n in range(len(GROUPS[half])):
            for r in range(1, PEERS):
                e_copy(n, half, r).wait_send()
    c_each(lambda k: c_copy(k, lon).wait_send())
    c_each(lambda k: c_copy(k, (lon + SECTORS - k) % SECTORS).wait_recv())
    cost_out[...] = jnp.sum(cost_all[...], axis=0)


def deliver(inc, adj, cost, inc_out, adj_out, cost_out, sem):
    copies = [
        pltpu.make_async_copy(src, dst, sem.at[n])
        for n, (src, dst) in enumerate(((inc, inc_out), (adj, adj_out), (cost, cost_out)))
    ]
    for copy in copies:
        copy.start()
    for copy in copies:
        copy.wait()


def body(
    field, ens, sdev, lon_taper, static_taper, loc_vert, static_vert, obs_block, obs_value, obs_rinv, obs_horiz, obs_vert
):
    members, slots = ens.shape[0], obs_block.shape[0]
    vmem = pl.BlockSpec(memory_space=pltpu.VMEM)
    hbm = pl.BlockSpec(memory_space=pltpu.HBM)
    dma = pltpu.SemaphoreType.DMA
    tile = (ROWS, 2, 8, 128)
    increment, adjoint, cost = pl.pallas_call(
        kernel,
        out_shape=(
            jax.ShapeDtypeStruct(tile, F32),
            jax.ShapeDtypeStruct(tile, F32),
            jax.ShapeDtypeStruct((1, 128), F32),
        ),
        in_specs=[hbm] * 12,
        out_specs=(vmem, vmem, vmem),
        scratch_shapes=[
            pltpu.VMEM((OWN, LEVELS, 6, 8, 128), BF16),
            pltpu.VMEM((LEVELS, 6, 8, 128), F32),
            pltpu.VMEM((LEVELS, 6, 8, 128), BF16),
            pltpu.VMEM((4, ROWS, LEVELS), BF16),
            pltpu.VMEM((4, 576, 256), BF16),
            pltpu.VMEM((128, 192), BF16),
            pltpu.VMEM((128, 192), BF16),
            pltpu.VMEM((576, 576), BF16),
            pltpu.VMEM((144, 576), BF16),
            pltpu.VMEM((4, LEVELS, 8, 128), F32),
            pltpu.VMEM((2, ROWS, 8, 128), F32),
            pltpu.VMEM((4, 2, ROWS, 8, 128), F32),
            pltpu.VMEM((2, 2, 2, ROWS, 8, 128), BF16),
            pltpu.VMEM((3, 2, ROWS, 8, 128), BF16),
            pltpu.VMEM(tile, F32),
            pltpu.VMEM(tile, F32),
            pltpu.VMEM((ROWS, LEVELS), BF16),
            pltpu.VMEM((1, 17), BF16),
            pltpu.VMEM((1, 17), BF16),
            pltpu.VMEM((1, slots), jnp.int32),
            pltpu.VMEM((1, slots), F32),
            pltpu.VMEM((1, slots), F32),
            pltpu.VMEM((slots, 128), F32),
            pltpu.VMEM((ROWS, slots), F32),
            pltpu.VMEM((16, slots), F32),
            pltpu.VMEM((slots, 256), BF16),
            pltpu.VMEM((256, slots), BF16),
            pltpu.VMEM((288, slots), BF16),
            pltpu.VMEM((288, slots), BF16),
            pltpu.VMEM((4, 1, slots), F32),
            pltpu.VMEM((SECTORS, 1, 128), F32),
            dma((4, 2, PEERS)),
            dma((4, 2, PEERS)),
            dma((OWN, 2)),
            dma((OWN, 2)),
            dma((2, PEERS)),
            dma((2, PEERS)),
            dma((2, 2)),
            dma((2, 2)),
            dma((4,)),
            dma((4,)),
            dma((4, 2)),
            dma((4, 2)),
            dma((3, 2)),
            dma((3, 2)),
            dma((4,)),
            dma((4,)),
            dma((SECTORS,)),
            dma((SECTORS,)),
            dma((11,)),
            pltpu.SemaphoreType.REGULAR((2,)),
        ],
        compiler_params=pltpu.CompilerParams(collective_id=0, has_side_effects=True, vmem_limit_bytes=48 * 1024 * 1024),
        name="members",
    )(
        *(
            pltpu.with_memory_space_constraint(x, pltpu.HBM)
            for x in (
                ens.reshape(members, *tile),
                field.reshape(tile),
                sdev.reshape(tile),
                lon_taper[None],
                static_taper[None],
                loc_vert,
                static_vert,
                obs_block[None],
                obs_value[None],
                obs_rinv[None],
                obs_horiz,
                obs_vert.T,
            )
        )
    )
    shapes = [jax.ShapeDtypeStruct(x.shape, F32) for x in (increment, adjoint, cost)]
    increment, adjoint, cost = pl.pallas_call(
        deliver,
        out_shape=shapes,
        in_specs=[vmem] * 3,
        out_specs=[hbm] * 3,
        scratch_shapes=[dma((3,))],
        compiler_params=pltpu.CompilerParams(vmem_limit_bytes=4 * 1024 * 1024),
        name="deliver",
    )(increment, adjoint, cost)
    return increment.reshape(field.shape), adjoint.reshape(field.shape), cost[0, 0]


def solution(mesh):
    return jax.shard_map(
        body,
        mesh=mesh,
        in_specs=(
            P("lev", "lon", None),
            P(None, "lev", "lon", None),
            P("lev", "lon", None),
            P(),
            P(),
            P("lev", None),
            P("lev", None),
            P("lon"),
            P("lon"),
            P("lon"),
            P("lon", None),
            P("lon", "lev"),
        ),
        out_specs=(P("lev", "lon", None), P("lev", "lon", None), P()),
        check_vma=False,
    )
```

```python
import functools

import jax
import jax.numpy as jnp
from jax import lax
from jax.experimental import pallas as pl
from jax.experimental.pallas import tpu as pltpu
from jax.sharding import PartitionSpec as P

MESH = pl.DeviceIdType.MESH
F32 = jnp.float32
BF16 = jnp.bfloat16

ens_weight = 0.8
static_weight = 0.5

COLUMNS = 16
PEERS = 8
SECTORS = 32
CHUNKS = 5
PAIR = 2
OWN = CHUNKS * PAIR
LEVELS = 72
ROWS = 18
QUADS = LEVELS // 4


def iota(shape, dim):
    return lax.broadcasted_iota(jnp.int32, shape, dim)


def band(taper, out):
    row, col = iota((128, 192), 0), iota((128, 192), 1)
    at = col % 48 - (row // 32) * 8 - row % 8
    same = (row // 8) % 4 == col // 48
    total = jnp.zeros((128, 192), F32)
    for d in range(17):
        total = total + jnp.where(at == d, taper[:, d : d + 1].astype(F32), 0.0)
    out[...] = jnp.where(same, total, 0.0).astype(BF16)


def spread(matrix):
    cols = (iota((LEVELS, 576), 0) == iota((LEVELS, 576), 1) // 8).astype(BF16)
    rows = (iota((144, ROWS), 0) // 8 == iota((144, ROWS), 1)).astype(BF16)
    wide = jnp.dot(matrix.astype(BF16), cols, preferred_element_type=F32).astype(BF16)
    tall = jnp.dot(rows, wide, preferred_element_type=F32)
    keep = iota((144, 576), 0) % 8 == iota((144, 576), 1) % 8
    return jnp.where(keep, tall, 0.0).astype(BF16)


def swapped(x):
    row, group = iota(x.shape, 1), iota(x.shape, 2) // 16
    for b in (1, 2, 4):
        row_bit, group_bit = (row // b) % 2, (group // b) % 2
        after = pltpu.roll(pltpu.roll(x, 8 - b, 1), 16 * b, 2)
        before = after if b == 4 else pltpu.roll(pltpu.roll(x, b, 1), 128 - 16 * b, 2)
        x = jnp.where(row_bit == group_bit, x, jnp.where(row_bit == 0, after, before))
    return x


def far_away(k):
    x, y, z = k // 8, (k // 2) % 4, k % 2
    return min(x, 4 - x) + min(y, 4 - y) + 2 * z


def halves(x):
    high = x.astype(BF16)
    return high, (x - high.astype(F32)).astype(BF16)


def kernel(
    ens, field, sdev, ltaper, staper, loc, svert, block, value, rinv, horiz, vert,
    inc_out, adj_out, cost_out,
    ens_buf, field_buf, spart_buf, loc_buf, zh_buf, band_e, band_s, vert_e, vert_s, acc, sv_buf,
    d_buf, r_out, r_buf,
    field_v, sdev_v, svert_v, ltaper_v, staper_v, block_v, value_v, rinv_v, horiz_v, vert_v,
    pick, h_cat, h_turned, spread_hi, spread_lo, hx_all, cost_all,
    es_send, es_recv, ey_send, ey_recv, f_send, f_recv, fy_send, fy_recv, l_send, l_recv,
    d_send, d_recv, r_send, r_recv, x_send, x_recv, c_send, c_recv, in_sem, known,
):
    lon, q = lax.axis_index("lon"), lax.axis_index("lev")
    column, h = lon // 2, lon % 2
    zlo, core = q // 2, q % 2
    px, py = lon // 8, (lon // 2) % 4
    left = 2 * ((column + COLUMNS - 1) % COLUMNS) + h
    right = 2 * ((column + 1) % COLUMNS) + h

    def peer(r):
        hr = 1 - h if r & 4 else h
        zr = 1 - zlo if r & 2 else zlo
        cr = 1 - core if r & 1 else core
        return hr, 2 * zr + cr

    def column_device(r):
        hr, qr = peer(r)
        return (2 * column + hr, qr)

    def y_device(k):
        return (8 * px + 2 * ((py + k) % 4) + h, q)

    def x_device(k):
        return (8 * ((px + k) % 4) + 2 * py + h, q)

    early = [(field, field_v), (sdev, sdev_v), (loc, loc_buf.at[q]), (svert, svert_v)]
    early += [(ltaper, ltaper_v), (staper, staper_v)]
    late = [(block, block_v), (value, value_v), (rinv, rinv_v), (horiz, horiz_v), (vert, vert_v)]
    loads = [pltpu.make_async_copy(src, dst, in_sem.at[n]) for n, (src, dst) in enumerate(early + late)]
    barrier = pltpu.get_barrier_semaphore()
    greeted = [column_device(r) for r in range(1, PEERS)] + [(left, q), (right, q)]
    greeted += [y_device(k) for k in (1, 2, 3)] + [x_device(k) for k in (1, 2, 3)]
    for device in greeted:
        pl.semaphore_signal(barrier, inc=1, device_id=device, device_id_type=MESH)

    for copy in loads[: len(early)]:
        copy.start()
    for copy in loads[: len(early)]:
        copy.wait()
    own = pl.ds(ROWS * q, ROWS)
    for i in range(2):
        spart_buf[own, 1 + 2 * h + i] = (sdev_v[:, i] * field_v[:, i]).astype(BF16)
        field_buf[own, 1 + 2 * h + i] = field_v[:, i]
    pl.semaphore_wait(barrier, len(greeted))

    def remote(src, dst, send, recv, where):
        return pltpu.make_async_remote_copy(
            src_ref=src, dst_ref=dst, send_sem=send, recv_sem=recv, device_id=where, device_id_type=MESH
        )

    bufs = (field_buf, spart_buf)

    def f_slot(n, r):
        hr, qr = peer(r)
        return bufs[n].at[pl.ds(ROWS * qr, ROWS), pl.ds(1 + 2 * hr, 2)]

    def f_half(n, r, i):
        hr, qr = peer(r)
        return bufs[n].at[pl.ds(ROWS * qr, ROWS), 1 + 2 * hr + i]

    def f_relay(n, r):
        half, sem, to = (0, 4, 2) if r == 6 else (1, 0, 6)
        slot = f_half(n, r, half)
        return remote(slot, slot, f_send.at[n, sem], f_recv.at[n, sem], column_device(to))

    def f_relayed(n):
        for half, sem, via in ((0, 4, 2), (1, 0, 6)):
            slot = f_half(n, 4, half)
            remote(slot, slot, f_send.at[n, sem], f_recv.at[n, sem], column_device(via)).wait_recv()

    def f_copy(n, r):
        src = field_v if n == 0 else f_slot(n, 0)
        return remote(src, f_slot(n, 0), f_send.at[n, r], f_recv.at[n, r], column_device(r))

    def f_pass(n, r):
        return remote(f_slot(n, r), f_slot(n, r), f_send.at[n, r + 1], f_recv.at[n, r + 1], column_device(1))

    def f_arrived(n, r):
        remote(f_slot(n, r), f_slot(n, r), f_send.at[n, r], f_recv.at[n, r], column_device(r)).wait_recv()

    def l_copy(r):
        return remote(loc_buf.at[q], loc_buf.at[q], l_send.at[r], l_recv.at[r], column_device(r))

    def l_arrived(r):
        hr, qr = peer(r)
        remote(loc_buf.at[qr], loc_buf.at[qr], l_send.at[r], l_recv.at[r], column_device(r)).wait_recv()

    def piece(n, half):
        if isinstance(n, int) and half == 1 and n >= CHUNKS - 1:
            return OWN - 2 + n - (CHUNKS - 1), 1
        return PAIR * n, PAIR

    def e_copy(n, half, r):
        hr, qr = peer(r)
        first, count = piece(n, half)
        here = h if half == 0 else 1 - h
        there = 1 + 3 * h if half == 0 else 2 + h
        src = ens.at[pl.ds(OWN * (4 * hr + qr) + first, count), :, here]
        dst = ens_buf.at[pl.ds(first, count), pl.ds(ROWS * q, ROWS), there]
        if r == 0:
            return pltpu.make_async_copy(src, dst, es_recv.at[n, half, 0])
        return remote(src, dst, es_send.at[n, half, r], es_recv.at[n, half, r], column_device(r))

    def e_arrived(n, half):
        first, count = piece(n, half)
        e_copy(n, half, 0).wait()
        for r in range(1, PEERS):
            hr, qr = peer(r)
            there = 1 + 3 * hr if half == 0 else 2 + hr
            slot = ens_buf.at[pl.ds(first, count), pl.ds(ROWS * qr, ROWS), there]
            remote(slot, slot, es_send.at[n, half, r], es_recv.at[n, half, r], column_device(r)).wait_recv()

    def sides(buf, send, recv, lead):
        mine = [buf.at[lead + (slice(None), 1)], buf.at[lead + (slice(None), 4)]]
        theirs = [buf.at[lead + (slice(None), 5)], buf.at[lead + (slice(None), 0)]]
        return [
            remote(mine[s], theirs[s], send.at[s], recv.at[s], ((left, right)[s], q)) for s in range(2)
        ]

    def e_sides(c):
        return [s for k in range(PAIR) for s in sides(ens_buf, ey_send.at[c, k], ey_recv.at[c, k], (PAIR * c + k,))]

    def f_sides():
        return sides(field_buf, fy_send.at[0], fy_recv.at[0], ()) + sides(
            spart_buf, fy_send.at[1], fy_recv.at[1], ()
        )

    order = (2, 6, 4, 3, 7, 5, 1)
    for n in range(2):
        for r in (6, 2, 1):
            f_copy(n, r).start()
    for r in (2, 3, 1):
        l_copy(r).start()

    def send_members(c, half):
        for r in order:
            e_copy(c, half, r).start()
        e_copy(c, half, 0).start()

    send_members(0, 0)
    for k in (1, 2, 3):
        pl.semaphore_signal(known.at[0], inc=1, device_id=x_device(k), device_id_type=MESH)
    for copy in loads[len(early) :]:
        copy.start()

    band(ltaper_v[...], band_e)
    band(staper_v[...], band_s)
    for n in range(2):
        for r in (6, 2):
            f_arrived(n, r)
            f_relay(n, r).start()
            f_pass(n, r).start()
    for c in range(1, CHUNKS):
        send_members(c, 0)
        send_members(c - 1, 1)
    send_members(CHUNKS - 1, 1)
    send_members(CHUNKS, 1)
    vert_s[...] = spread(svert_v[...])
    vert_e[pl.ds(144 * q, 144)] = spread(loc_buf[q])
    for r in (1, 2, 3):
        l_arrived(r)
        hr, qr = peer(r)
        vert_e[pl.ds(144 * qr, 144)] = spread(loc_buf[qr])
    acc[...] = jnp.zeros_like(acc)

    pl.semaphore_wait(known.at[0], 3)
    hr, qr = peer(4)
    pl.semaphore_signal(known.at[1], inc=1, device_id=(2 * column + hr, qr), device_id_type=MESH)
    for n in range(2):
        f_relayed(n)
        f_pass(n, 4).start()
    pl.semaphore_wait(known.at[1], 1)
    for n in range(2):
        for r in (1, 3, 7, 5):
            f_arrived(n, r)
    for s in f_sides():
        s.start()
    e_arrived(0, 0)
    for s in e_sides(0):
        s.start()

    for copy in loads[len(early) :]:
        copy.wait()
    slots = block_v.shape[1]
    local = block_v[...] - lon * 16
    pick[...] = ((iota((16, slots), 0) == local) & (block_v[...] >= 0)).astype(F32)
    high, low = halves(horiz_v[...])
    h_cat[:, :128] = high
    h_cat[:, 128:] = low
    high, low = halves(horiz_v[...].T)
    h_turned[:128] = high
    h_turned[128:] = low

    def smooth(weights, read):
        def quad(n, _):
            out_rows = jnp.dot(weights[...], read(4 * n), preferred_element_type=F32).astype(BF16)
            lanes = out_rows.shape[1]
            for ib in range(4):
                zh_buf[ib, pl.ds(pl.multiple_of(32 * n, 32), 32), :lanes] = out_rows[32 * ib : 32 * ib + 32]
            return 0

        lax.fori_loop(0, QUADS, quad, 0, unroll=9)

    def read_static(m):
        return spart_buf[pl.ds(m, 4)].astype(F32).reshape(192, 128).astype(BF16)

    def smooth_members(c):
        def read(m):
            weight = field_buf[pl.ds(m, 4)]
            both = [(ens_buf[PAIR * c + k, pl.ds(m, 4)].astype(F32) * weight).reshape(192, 128) for k in range(PAIR)]
            return jnp.concatenate(both, axis=1).astype(BF16)

        smooth(band_e, read)

    def mix(c, ib, third):
        rows = pl.ds(pl.multiple_of(192 * third, 192), 192)
        levels = pl.ds(24 * third, 24)
        mixed = jnp.dot(vert_e[rows], zh_buf[ib], preferred_element_type=F32)
        total = acc[ib, levels]
        for k in range(PAIR):
            part = mixed[:, 128 * k : 128 * k + 128].reshape(24, 8, 128)
            total = total + ens_buf[PAIR * c + k, levels, 1 + ib].astype(F32) * part
        acc[ib, levels] = total
        return 0

    def smooth_one(k):
        def pair_of_quads(n, _):
            both = [
                (ens_buf[k, pl.ds(8 * n + 4 * g, 4)].astype(F32) * field_buf[pl.ds(8 * n + 4 * g, 4)]).reshape(192, 128)
                for g in range(2)
            ]
            rows = jnp.concatenate(both, axis=1).astype(BF16)
            out_rows = jnp.dot(band_e[...], rows, preferred_element_type=F32).astype(BF16)
            for ib in range(4):
                lanes = slice(128 * (ib % 2), 128 * (ib % 2) + 128)
                for g in range(2):
                    at = pl.ds(pl.multiple_of(64 * n + 32 * g, 32), 32)
                    zh_buf[ib // 2, at, lanes] = out_rows[32 * ib : 32 * ib + 32, 128 * g : 128 * g + 128]
            return 0

        lax.fori_loop(0, QUADS // 2, pair_of_quads, 0, unroll=9)

    def mix_one(k, side, third):
        rows = pl.ds(pl.multiple_of(192 * third, 192), 192)
        levels = pl.ds(24 * third, 24)
        mixed = jnp.dot(vert_e[rows], zh_buf[side], preferred_element_type=F32)
        for i in range(2):
            part = mixed[:, 128 * i : 128 * i + 128].reshape(24, 8, 128)
            tile_at = 2 * side + i
            acc[tile_at, levels] = acc[tile_at, levels] + ens_buf[k, levels, 1 + tile_at].astype(F32) * part
        return 0

    for s in f_sides():
        s.wait()
    smooth(band_s, read_static)
    for i in range(2):
        sv = jnp.dot(vert_s[...], zh_buf[2 * h + i, :, :128], preferred_element_type=F32)
        sv_buf[i] = static_weight * sdev_v[:, i] * sv.reshape(ROWS, 8, 128)

    def chunk(c, _):
        e_arrived(c + 1, 0)
        for s in e_sides(c + 1):
            s.start()
        e_arrived(c, 1)
        for s in e_sides(c):
            s.wait()
        smooth_members(c)
        lax.fori_loop(0, 12, lambda n, _: mix(c, n // 3, n % 3), 0, unroll=12)
        return 0

    last = CHUNKS - 1
    lax.fori_loop(0, last, chunk, 0)

    def tile(n):
        return (2 * (1 - h) + n) % 4

    def d_copy(n, far):
        there = 2 * (1 - zlo if far else zlo) + 1 - core
        src = acc.at[tile(n), pl.ds(ROWS * there, ROWS)]
        return remote(src, d_buf.at[n, far], d_send.at[n, far], d_recv.at[n, far], column_device(1))

    def r_copy(slot, i):
        src = r_out.at[(0, 0, 1)[slot], (0, 1, 1)[slot], i]
        return remote(src, r_buf.at[slot, i], r_send.at[slot, i], r_recv.at[slot, i], column_device((4, 6, 2)[slot]))

    def reduce(n):
        for far in range(2):
            d_copy(n, far).wait_recv()
        for far in range(2):
            if n >= 2 and far == 0:
                continue
            rows = pl.ds(ROWS * (2 * (1 - zlo if far else zlo) + core), ROWS)
            r_out[n // 2, far, n % 2] = (acc[tile(n), rows] + d_buf[n, far]).astype(BF16)
        for slot in (0, 1) if n < 2 else (2,):
            r_copy(slot, n % 2).start()

    e_arrived(last, 1)
    for s in e_sides(last):
        s.wait()
    smooth_one(OWN - 2)
    lax.fori_loop(0, 6, lambda n, _: mix_one(OWN - 2, n // 3, n % 3), 0, unroll=6)
    e_arrived(last + 1, 1)
    smooth_one(OWN - 1)
    for turn in range(2):
        side = 1 - h if turn == 0 else h
        lax.fori_loop(0, 3, lambda third, _: mix_one(OWN - 1, side, third), 0, unroll=3)
        for n in (2 * turn, 2 * turn + 1):
            for far in range(2):
                d_copy(n, far).start()
        if turn:
            reduce(0)
            reduce(1)
    reduce(2)
    reduce(3)
    for i in range(2):
        total = acc[2 * h + i, own] + d_buf[2 + i, 0]
        for slot in range(3):
            r_copy(slot, i).wait_recv()
            total = total + r_buf[slot, i].astype(F32)
        inc_out[:, i] = ens_weight * total + sv_buf[i]

    cells = swapped(inc_out[...].reshape(36, 8, 128)).reshape(288, 128)
    high, low = halves(cells)
    projected = jnp.dot(jnp.concatenate([high, high], axis=1), h_turned[...], preferred_element_type=F32)
    projected = projected + jnp.dot(low, h_turned[:128], preferred_element_type=F32)
    total = jnp.zeros((16, slots), F32)
    for l in range(ROWS):
        total = total + vert_v[l : l + 1] * projected[16 * l : 16 * l + 16]
    hx_all[q] = jnp.sum(total * pick[...], axis=0, keepdims=True)

    def x_copy(r):
        return remote(hx_all.at[q], hx_all.at[q], x_send.at[r], x_recv.at[r], column_device(r))

    for r in (2, 3, 1):
        x_copy(r).start()
    for r in (1, 2, 3):
        hr, qr = peer(r)
        remote(hx_all.at[qr], hx_all.at[qr], x_send.at[r], x_recv.at[r], column_device(r)).wait_recv()
    miss = hx_all[0] + hx_all[1] + hx_all[2] + hx_all[3] - value_v[...]
    dep = jnp.where(block_v[...] >= 0, rinv_v[...] * miss, 0.0)
    cost = jnp.sum(0.5 * dep * miss, axis=1, keepdims=True)

    def c_copy(k, slot):
        other = lon + k
        where = (jnp.where(other >= SECTORS, other - SECTORS, other), q)
        return remote(cost_all.at[slot], cost_all.at[slot], c_send.at[k], c_recv.at[k], where)

    def c_each(act):
        def one(k, _):
            act(k)
            return 0

        lax.fori_loop(1, SECTORS, one, 0)

    cost_all[lon] = jnp.broadcast_to(cost, (1, 128))
    for k in sorted(range(1, SECTORS), key=lambda k: -far_away(k)):
        c_copy(k, lon).start()

    weights = dep * pick[...]
    for l in range(ROWS):
        high, low = halves(vert_v[l : l + 1] * weights)
        spread_hi[16 * l : 16 * l + 16] = high
        spread_lo[16 * l : 16 * l + 16] = low


    both = jnp.dot(spread_hi[...], h_cat[...], preferred_element_type=F32)
    adjoint = both[:, :128] + both[:, 128:]
    adjoint = adjoint + jnp.dot(spread_lo[...], h_cat[:, :128], preferred_element_type=F32)
    adj_out[...] = swapped(adjoint.reshape(36, 8, 128)).reshape(ROWS, 2, 8, 128)


    for n in range(4):
        for far in range(2):
            d_copy(n, far).wait_send()
    for slot in range(3):
        for i in range(2):
            r_copy(slot, i).wait_send()
    for r in (1, 2, 3):
        l_copy(r).wait_send()
        x_copy(r).wait_send()
    for n in range(2):
        for r in (1, 2, 6):
            f_copy(n, r).wait_send()
        for r in (2, 6):
            f_relay(n, r).wait_send()
        for r in (2, 4, 6):
            f_pass(n, r).wait_send()

    def sent(c, _):
        for half in range(2):
            for r in range(1, PEERS):
                e_copy(c, half, r).wait_send()
        return 0

    lax.fori_loop(0, CHUNKS - 1, sent, 0)
    for r in range(1, PEERS):
        e_copy(CHUNKS - 1, 0, r).wait_send()
        e_copy(CHUNKS - 1, 1, r).wait_send()
        e_copy(CHUNKS, 1, r).wait_send()
    c_each(lambda k: c_copy(k, lon).wait_send())
    for k in sorted(range(1, SECTORS), key=far_away):
        c_copy(k, jnp.where(lon >= k, lon - k, lon + SECTORS - k)).wait_recv()
    cost_out[...] = jnp.sum(cost_all[...], axis=0)


def deliver(inc, adj, cost, inc_out, adj_out, cost_out, sem):
    copies = [
        pltpu.make_async_copy(src, dst, sem.at[n])
        for n, (src, dst) in enumerate(((inc, inc_out), (adj, adj_out), (cost, cost_out)))
    ]
    for copy in copies:
        copy.start()
    for copy in copies:
        copy.wait()


def body(
    field, ens, sdev, lon_taper, static_taper, loc_vert, static_vert, obs_block, obs_value, obs_rinv, obs_horiz, obs_vert
):
    members, slots = ens.shape[0], obs_block.shape[0]
    vmem = pl.BlockSpec(memory_space=pltpu.VMEM)
    hbm = pl.BlockSpec(memory_space=pltpu.HBM)
    dma = pltpu.SemaphoreType.DMA
    tile = (ROWS, 2, 8, 128)
    increment, adjoint, cost = pl.pallas_call(
        kernel,
        out_shape=(
            jax.ShapeDtypeStruct(tile, F32),
            jax.ShapeDtypeStruct(tile, F32),
            jax.ShapeDtypeStruct((1, 128), F32),
        ),
        in_specs=[hbm] * 12,
        out_specs=(vmem, vmem, vmem),
        scratch_shapes=[
            pltpu.VMEM((OWN, LEVELS, 6, 8, 128), BF16),
            pltpu.VMEM((LEVELS, 6, 8, 128), F32),
            pltpu.VMEM((LEVELS, 6, 8, 128), BF16),
            pltpu.VMEM((4, ROWS, LEVELS), BF16),
            pltpu.VMEM((4, 576, 256), BF16),
            pltpu.VMEM((128, 192), BF16),
            pltpu.VMEM((128, 192), BF16),
            pltpu.VMEM((576, 576), BF16),
            pltpu.VMEM((144, 576), BF16),
            pltpu.VMEM((4, LEVELS, 8, 128), F32),
            pltpu.VMEM((2, ROWS, 8, 128), F32),
            pltpu.VMEM((4, 2, ROWS, 8, 128), F32),
            pltpu.VMEM((2, 2, 2, ROWS, 8, 128), BF16),
            pltpu.VMEM((3, 2, ROWS, 8, 128), BF16),
            pltpu.VMEM(tile, F32),
            pltpu.VMEM(tile, F32),
            pltpu.VMEM((ROWS, LEVELS), BF16),
            pltpu.VMEM((1, 17), BF16),
            pltpu.VMEM((1, 17), BF16),
            pltpu.VMEM((1, slots), jnp.int32),
            pltpu.VMEM((1, slots), F32),
            pltpu.VMEM((1, slots), F32),
            pltpu.VMEM((slots, 128), F32),
            pltpu.VMEM((ROWS, slots), F32),
            pltpu.VMEM((16, slots), F32),
            pltpu.VMEM((slots, 256), BF16),
            pltpu.VMEM((256, slots), BF16),
            pltpu.VMEM((288, slots), BF16),
            pltpu.VMEM((288, slots), BF16),
            pltpu.VMEM((4, 1, slots), F32),
            pltpu.VMEM((SECTORS, 1, 128), F32),
            dma((CHUNKS + 1, 2, PEERS)),
            dma((CHUNKS + 1, 2, PEERS)),
            dma((CHUNKS, PAIR, 2)),
            dma((CHUNKS, PAIR, 2)),
            dma((2, PEERS)),
            dma((2, PEERS)),
            dma((2, 2)),
            dma((2, 2)),
            dma((4,)),
            dma((4,)),
            dma((4, 2)),
            dma((4, 2)),
            dma((3, 2)),
            dma((3, 2)),
            dma((4,)),
            dma((4,)),
            dma((SECTORS,)),
            dma((SECTORS,)),
            dma((11,)),
            pltpu.SemaphoreType.REGULAR((2,)),
        ],
        compiler_params=pltpu.CompilerParams(collective_id=0, has_side_effects=True, vmem_limit_bytes=48 * 1024 * 1024),
        name="members",
    )(
        *(
            pltpu.with_memory_space_constraint(x, pltpu.HBM)
            for x in (
                ens.reshape(members, *tile),
                field.reshape(tile),
                sdev.reshape(tile),
                lon_taper[None],
                static_taper[None],
                loc_vert,
                static_vert,
                obs_block[None],
                obs_value[None],
                obs_rinv[None],
                obs_horiz,
                obs_vert.T,
            )
        )
    )
    shapes = [jax.ShapeDtypeStruct(x.shape, F32) for x in (increment, adjoint, cost)]
    increment, adjoint, cost = pl.pallas_call(
        deliver,
        out_shape=shapes,
        in_specs=[vmem] * 3,
        out_specs=[hbm] * 3,
        scratch_shapes=[dma((3,))],
        compiler_params=pltpu.CompilerParams(vmem_limit_bytes=4 * 1024 * 1024),
        name="deliver",
    )(increment, adjoint, cost)
    return increment.reshape(field.shape), adjoint.reshape(field.shape), cost[0, 0]


def solution(mesh):
    return jax.shard_map(
        body,
        mesh=mesh,
        in_specs=(
            P("lev", "lon", None),
            P(None, "lev", "lon", None),
            P("lev", "lon", None),
            P(),
            P(),
            P("lev", None),
            P("lev", None),
            P("lon"),
            P("lon"),
            P("lon"),
            P("lon", None),
            P("lon", "lev"),
        ),
        out_specs=(P("lev", "lon", None), P("lev", "lon", None), P()),
        check_vma=False,
    )
```
